32 devices in a mesh: groups: 2 (over y), graph: 16 (over z, x, core).
Axes of the slice: x: 2, y: 2, z: 4, core: 2. Of those that a mesh axis runs over, the one named last changes fastest.
Arguments:
- edge_state: bfloat16 [8192, 512], P(('groups', 'graph')), parts along dimension 0, may hold values from -6 to 6
- atom_state: bfloat16 [512, 256], P(('groups', 'graph')), parts along dimension 0, may hold values from -6 to 6
- atom_sends: int32 [4096], P(('groups', 'graph')), parts along dimension 0, may hold values from 0 to 15
- edge_source: int32 [8192], P(('groups', 'graph')), parts along dimension 0, may hold values from 0 to 127
- edge_target: int32 [8192], P(('groups', 'graph')), parts along dimension 0, may hold values from 0 to 15
- send_edges: int32 [262144], P(('groups', 'graph')), parts along dimension 0, may hold values from 0 to 255
- triplet_in: int32 [262144], P(('groups', 'graph')), parts along dimension 0, may hold values from 0 to 8191, as said below
- triplet_out: int32 [262144], P(('groups', 'graph')), parts along dimension 0, may hold values from 0 to 8191, as said below
- triplet_valid: int32 [262144], P(('groups', 'graph')), parts along dimension 0, may hold values 0 or 1
- triplet_basis: bfloat16 [16, 262144], P(None, ('groups', 'graph')), parts along dimension 1, may hold values from -6 to 6
- return_edges: int32 [262144], P(('groups', 'graph')), parts along dimension 0, may hold values from 0 to 255
- w_edge: bfloat16 [512, 512], replicated, may hold values from -0.25 to 0.25
- w_source: bfloat16 [256, 512], replicated, may hold values from -0.375 to 0.375
- w_down: bfloat16 [512, 64], replicated, may hold values from -0.25 to 0.25
- w_bilinear: bfloat16 [64, 1024], replicated, may hold values from -0.1875 to 0.1875
- w_up: bfloat16 [64, 512], replicated, may hold values from -0.125 to 0.125
- w_residual: bfloat16 [4, 512, 512], replicated, may hold values from -0.25 to 0.25
- w_atom: bfloat16 [512, 256], replicated, may hold values from -0.25 to 0.25
Outputs:
- edge_out: bfloat16 [8192, 512], P(('groups', 'graph')), parts along dimension 0
- atom_out: bfloat16 [512, 256], P(('groups', 'graph')), parts along dimension 0
The draws below stay inside these ranges and needn't reach their ends.
There are 2 independent parts, one for each index of `groups`. The reference program is written for one: setup_inputs(seed, part) draws one part's arguments, and reference() takes and returns one part's arrays. A program takes and returns all parts, laid end to end along the dimension named above; an argument that names none is the same for every part. Nothing has to cross between parts.
Inputs may be any that keep to these rules, and one draw needn't show every extreme that they name: `atom_sends`: entry d * 8 + c of a device's 128 entries is sent to device d. `send_edges`: entry t * 512 + c of a device's 8192 entries is sent to tile t. `triplet_in`: triplet j of a tile reads a received slot in the same aligned block of 512 slots as j. `triplet_out`: slot d * 512 + c of a tile is returned to device d; triplet j of a tile adds to a slot in the same aligned block of 512 slots as j. `return_edges`: entry t * 512 + c of a device's 8192 entries belongs to the slot that tile t returns in place c.
All inputs are finite; a program needn't handle non-finite values. No bound on the sum of `triplet_valid` on one device may be relied on, other than what follows from the above.
Results may differ from the reference program's by a relative error of at most 0.0095.
Values may be sent and summed in bfloat16 or wider, within the bound.
A program may use at most 64 MiB of HBM per device.

```python
import jax
import jax.numpy as jnp
from jax import lax

DE = 512
DA = 256
DP = 64
NB = 16
E_DEV = 256
TPE = 32
WIN = 512
ATOM_DEV = 16
EDGES = 4096
ATOMS = 256
TRIP_DEV = 8192
TRIPLETS = 131072
CAP = 512
ASLOTS = 128
CAP_A = 8
ASENDS = 2048
N_GRAPH = 16


def block_slots(key):
    positions = jnp.arange(TRIPLETS, dtype=jnp.int32) % TRIP_DEV
    starts = positions // WIN * WIN
    return starts + jax.random.randint(key, (TRIPLETS,), 0, WIN, dtype=jnp.int32)


def draw_triplet_in(key, part):
    return block_slots(jax.random.fold_in(key, 101))


def draw_triplet_out(key, part):
    return block_slots(jax.random.fold_in(key, 202))


def touch_ends(entries, key, smallest, high):
    longest = entries.shape.index(max(entries.shape))
    spots = []
    for shift in (0, 1):
        where = [jax.random.randint(jax.random.fold_in(key, axis), (), 0, length) for axis, length in enumerate(entries.shape)]
        where[longest] = (where[longest] + shift) % entries.shape[longest]
        spots.append(tuple(where))
    return entries.at[spots[0]].set(smallest).at[spots[1]].set(high)


def block_levels(own_key, dims, cuts, low, top_value):
    factor_of, own = 1.0, jax.random.fold_in(own_key, 6)
    for dim, shards_of in cuts:
        steps = jnp.exp(jax.random.uniform(jax.random.fold_in(own, dim), (shards_of,), jnp.float32, low / len(cuts), top_value / len(cuts)))
        factor_of = factor_of * jnp.repeat(steps, dims[dim] // shards_of).reshape([-1 if axis == dim else 1 for axis in range(len(dims))])
    return factor_of


def bell_draw(rng, dims, scale, most, pieces=(), kind=jnp.bfloat16):
    gain = block_levels(rng, dims, pieces, -0.22, 0.18) if pieces else 1.0
    entries = jax.random.normal(rng, dims, jnp.float32) * scale * gain
    return jnp.minimum(jnp.maximum(entries, -most), most).astype(kind)


def setup_inputs(seed: int = 0, part: int = 0) -> dict:
    streams_of = jax.random.split(jax.random.key(seed), 19)
    own_keys = jax.random.split(jax.random.fold_in(streams_of[18], part), 19)
    return {
        "edge_state": bell_draw(own_keys[0], (EDGES, DE), 1.0, 6.0, ((0, 16),)),
        "atom_state": bell_draw(own_keys[1], (ATOMS, DA), 1.0, 6.0, ((0, 16),)),
        "atom_sends": touch_ends(jax.random.randint(own_keys[2], (ASENDS,), 0, ATOM_DEV), jax.random.fold_in(own_keys[2], 1), 0, ATOM_DEV - 1).astype(jnp.int32),
        "edge_source": touch_ends(jax.random.randint(own_keys[3], (EDGES,), 0, ASLOTS), jax.random.fold_in(own_keys[3], 1), 0, ASLOTS - 1).astype(jnp.int32),
        "edge_target": touch_ends(jax.random.randint(own_keys[4], (EDGES,), 0, ATOM_DEV), jax.random.fold_in(own_keys[4], 1), 0, ATOM_DEV - 1).astype(jnp.int32),
        "send_edges": touch_ends(jax.random.randint(own_keys[5], (TRIPLETS,), 0, E_DEV), jax.random.fold_in(own_keys[5], 1), 0, E_DEV - 1).astype(jnp.int32),
        "triplet_in": draw_triplet_in(jax.random.fold_in(jax.random.fold_in(streams_of[18], part), 71), part),
        "triplet_out": draw_triplet_out(jax.random.fold_in(jax.random.fold_in(streams_of[18], part), 71), part),
        "triplet_valid": touch_ends((jax.random.randint(own_keys[8], (TRIPLETS,), 0, 4) < 3).astype(jnp.int32), jax.random.fold_in(own_keys[8], 1), 0, 1),
        "triplet_basis": bell_draw(own_keys[9], (NB, TRIPLETS), 1.0, 6.0, ((1, 16),)),
        "return_edges": touch_ends(jax.random.randint(own_keys[10], (TRIPLETS,), 0, E_DEV), jax.random.fold_in(own_keys[10], 1), 0, E_DEV - 1).astype(jnp.int32),
        "w_edge": bell_draw(streams_of[11], (DE, DE), DE ** -0.5, 0.25),
        "w_source": bell_draw(streams_of[12], (DA, DE), DA ** -0.5, 0.375),
        "w_down": bell_draw(streams_of[13], (DE, DP), DE ** -0.5, 0.25),
        "w_bilinear": bell_draw(streams_of[14], (DP, NB * DP), (DP * NB) ** -0.5, 0.1875),
        "w_up": bell_draw(streams_of[15], (DP, DE), (DP * TPE) ** -0.5, 0.125),
        "w_residual": bell_draw(streams_of[16], (4, DE, DE), DE ** -0.5, 0.25),
        "w_atom": bell_draw(streams_of[17], (DE, DA), DE ** -0.5, 0.25),
    }


inv_root = 0.7071067811865476


def matmul(left, right):
    return jnp.dot(left, right, preferred_element_type=jnp.float32)


def bilinear_terms(inputs_x, coeffs, keeps, w_bilinear):
    expanded = matmul(inputs_x, w_bilinear)
    expanded = expanded.reshape(inputs_x.shape[0], coeffs.shape[0], -1)
    mixed = jnp.einsum("tkd,kt->td", expanded, coeffs.astype(jnp.float32))
    return mixed * keeps.astype(jnp.float32)[:, None]


def slot_table(indices, peer_count, width, shift):
    offsets = (jnp.arange(peer_count, dtype=jnp.int32) * shift)[:, None, None]
    shaped = indices.reshape(peer_count, peer_count, width) + offsets
    return jnp.transpose(shaped, (1, 0, 2)).reshape(peer_count, peer_count * width)


def reference(edge_state, atom_state, atom_sends, edge_source, edge_target, send_edges, triplet_in, triplet_out, triplet_valid, triplet_basis, return_edges, w_edge, w_source, w_down, w_bilinear, w_up, w_residual, w_atom):
    peer_count = N_GRAPH
    atom_slots = slot_table(atom_sends, peer_count, CAP_A, ATOM_DEV)
    source_ids = jnp.take_along_axis(atom_slots, edge_source.reshape(peer_count, E_DEV), axis=1).reshape(-1)
    src_rows = atom_state[source_ids]
    pre_act = matmul(edge_state, w_edge) + matmul(src_rows, w_source)
    activated = jax.nn.silu(pre_act).astype(jnp.bfloat16)
    projected = jax.nn.silu(matmul(activated, w_down)).astype(jnp.bfloat16)
    edge_slots = slot_table(send_edges, peer_count, CAP, E_DEV)
    back_slots = slot_table(return_edges, peer_count, CAP, E_DEV)

    def tile_work(operands):
        slot_ids, local_in, local_out, keeps, coeffs = operands
        inputs_x = projected[slot_ids[local_in]]
        mixed = bilinear_terms(inputs_x, coeffs, keeps, w_bilinear)
        summed = jnp.zeros((TRIP_DEV, DP), jnp.float32).at[local_out].add(mixed)
        return summed.astype(jnp.bfloat16)

    basis_tiles = jnp.transpose(triplet_basis.reshape(NB, peer_count, TRIP_DEV), (1, 0, 2))
    slot_sums = lax.map(tile_work, (edge_slots, triplet_in.reshape(peer_count, TRIP_DEV), triplet_out.reshape(peer_count, TRIP_DEV), triplet_valid.reshape(peer_count, TRIP_DEV), basis_tiles))
    aggregate = jnp.zeros((EDGES, DP), jnp.float32).at[back_slots.reshape(-1)].add(slot_sums.reshape(-1, DP).astype(jnp.float32))
    aggregate = aggregate.astype(jnp.bfloat16)
    update = jax.nn.silu(matmul(aggregate, w_up))
    base = ((edge_state.astype(jnp.float32) + activated.astype(jnp.float32)) * inv_root).astype(jnp.bfloat16)
    inner_one = jax.nn.silu(matmul(base, w_residual[0])).astype(jnp.bfloat16)
    middle = ((base.astype(jnp.float32) + jax.nn.silu(matmul(inner_one, w_residual[1]))) * inv_root).astype(jnp.bfloat16)
    inner_two = jax.nn.silu(matmul(middle, w_residual[2])).astype(jnp.bfloat16)
    chain = (middle.astype(jnp.float32) + jax.nn.silu(matmul(inner_two, w_residual[3]))) * inv_root
    edge_out = (chain + update).astype(jnp.bfloat16)
    contrib = matmul(edge_out, w_atom).astype(jnp.bfloat16)
    targets = edge_target + (jnp.arange(EDGES, dtype=jnp.int32) // E_DEV) * ATOM_DEV
    atom_sum = jnp.zeros((ATOMS, DA), jnp.float32).at[targets].add(contrib.astype(jnp.float32))
    atom_out = (atom_state.astype(jnp.float32) + jax.nn.silu(0.25 * atom_sum)).astype(jnp.bfloat16)
    return edge_out, atom_out
```

```python
import functools

import jax
import jax.numpy as jnp
from jax import lax
from jax.experimental import pallas as pl
from jax.experimental.pallas import tpu as pltpu
from jax.sharding import PartitionSpec as P

WIN = 512
APARTS = 1
UNROLL = False


inv_root = 0.7071067811865476


def matmul(left, right):
    return jnp.dot(left, right, preferred_element_type=jnp.float32)


def pick_rows(indices, table):
    chooser = (indices[:, None] == jnp.arange(table.shape[0], dtype=jnp.int32)[None, :]).astype(
        table.dtype
    )
    return matmul(chooser, table).astype(table.dtype)


def bilinear_terms(inputs_x, coeffs, keeps, w_bilinear):
    expanded = matmul(inputs_x, w_bilinear)
    expanded = expanded.reshape(inputs_x.shape[0], coeffs.shape[0], -1)
    mixed = jnp.einsum("tkd,kt->td", expanded, coeffs.astype(jnp.float32))
    return mixed * keeps.astype(jnp.float32)[:, None]


def tile_sums(slot_rows, local_in, local_out, keeps, coeffs, w_bilinear):
    trip_count = slot_rows.shape[0]
    block_size = WIN
    block_count = trip_count // block_size
    basis_rows = coeffs.shape[0]
    block_iota = jnp.arange(block_size, dtype=jnp.int32)

    def one_block(operands):
        rows_blk, in_blk, out_blk, keep_blk, coef_blk = operands
        in_hot = ((in_blk % block_size)[:, None] == block_iota[None, :]).astype(jnp.bfloat16)
        inputs_x = matmul(in_hot, rows_blk).astype(jnp.bfloat16)
        mixed = bilinear_terms(inputs_x, coef_blk, keep_blk, w_bilinear)
        out_hot = (block_iota[:, None] == (out_blk % block_size)[None, :]).astype(jnp.float32)
        return jnp.dot(
            out_hot, mixed, precision=lax.Precision.HIGHEST, preferred_element_type=jnp.float32
        )

    shaped_coeffs = jnp.transpose(coeffs.reshape(basis_rows, block_count, block_size), (1, 0, 2))
    summed = lax.map(
        one_block,
        (
            slot_rows.reshape(block_count, block_size, -1),
            local_in.reshape(block_count, block_size),
            local_out.reshape(block_count, block_size),
            keeps.reshape(block_count, block_size),
            shaped_coeffs,
        ),
    )
    return summed.reshape(trip_count, -1).astype(jnp.bfloat16)


def plain_on_device(
    edge_state,
    atom_state,
    atom_sends,
    edge_source,
    edge_target,
    send_edges,
    triplet_in,
    triplet_out,
    triplet_valid,
    triplet_basis,
    return_edges,
    w_edge,
    w_source,
    w_down,
    w_bilinear,
    w_up,
    w_residual,
    w_atom,
):
    edge_count = edge_state.shape[0]
    atom_count = atom_state.shape[0]
    arrived_atoms = lax.all_to_all(
        pick_rows(atom_sends, atom_state), "graph", split_axis=0, concat_axis=0, tiled=True
    )
    src_rows = pick_rows(edge_source, arrived_atoms)
    pre_act = matmul(edge_state, w_edge) + matmul(src_rows, w_source)
    activated = jax.nn.silu(pre_act).astype(jnp.bfloat16)
    projected = jax.nn.silu(matmul(activated, w_down)).astype(jnp.bfloat16)
    slot_rows = lax.all_to_all(
        pick_rows(send_edges, projected), "graph", split_axis=0, concat_axis=0, tiled=True
    )
    slot_sums = tile_sums(
        slot_rows, triplet_in, triplet_out, triplet_valid, triplet_basis, w_bilinear
    )
    returned = lax.all_to_all(slot_sums, "graph", split_axis=0, concat_axis=0, tiled=True)
    back_hot = (jnp.arange(edge_count, dtype=jnp.int32)[:, None] == return_edges[None, :]).astype(
        jnp.bfloat16
    )
    aggregate = matmul(back_hot, returned)
    update = jax.nn.silu(matmul(aggregate.astype(jnp.bfloat16), w_up))
    base = ((edge_state.astype(jnp.float32) + activated.astype(jnp.float32)) * inv_root).astype(
        jnp.bfloat16
    )
    inner_one = jax.nn.silu(matmul(base, w_residual[0])).astype(jnp.bfloat16)
    middle = (
        (base.astype(jnp.float32) + jax.nn.silu(matmul(inner_one, w_residual[1]))) * inv_root
    ).astype(jnp.bfloat16)
    inner_two = jax.nn.silu(matmul(middle, w_residual[2])).astype(jnp.bfloat16)
    chain = (middle.astype(jnp.float32) + jax.nn.silu(matmul(inner_two, w_residual[3]))) * inv_root
    edge_out = (chain + update).astype(jnp.bfloat16)
    contrib = matmul(edge_out, w_atom).astype(jnp.bfloat16)
    one_hot = (edge_target[None, :] == jnp.arange(atom_count, dtype=jnp.int32)[:, None]).astype(
        jnp.bfloat16
    )
    atom_sum = matmul(one_hot, contrib)
    atom_out = (atom_state.astype(jnp.float32) + jax.nn.silu(0.25 * atom_sum)).astype(jnp.bfloat16)
    return (edge_out, atom_out)


def silu(value):
    half = 0.5 * value
    return half + half * jnp.tanh(half)


def dot_at(left, right, left_dim, right_dim):
    return lax.dot_general(
        left, right, (((left_dim,), (right_dim,)), ((), ())), preferred_element_type=jnp.float32
    )


def hot_columns(row_count, indices):
    rows = lax.broadcasted_iota(jnp.int32, (row_count, indices.shape[1]), 0)
    return jnp.where(rows == indices, 1.0, 0.0).astype(jnp.bfloat16)


def partner(me, step, n):
    peer = me
    bit = 1
    while bit < n:
        mine = lax.rem(lax.div(me, bit), 2)
        flip = (step // bit) % 2 if isinstance(step, int) else lax.rem(lax.div(step, bit), 2)
        peer = peer + flip * (1 - 2 * mine) * bit
        bit *= 2
    return peer


def look_up(table, indices):
    lanes = indices.shape[1]
    found = []
    for row in range(indices.shape[0]):
        wanted = jnp.broadcast_to(indices[row : row + 1, :], (8, lanes))
        lane = wanted & (lanes - 1)
        value = jnp.zeros_like(wanted)
        for first in range(0, table.shape[1], lanes):
            part = jnp.take_along_axis(
                jnp.broadcast_to(table[:, first : first + lanes], (8, lanes)),
                lane,
                axis=1,
                mode="promise_in_bounds",
            )
            value = jnp.where(wanted - lane == first, part, value)
        found.append(value)
    return jnp.concatenate(found, axis=1)


def hot_from(row_count, eight_rows):
    lanes = eight_rows.shape[1]
    sixteen = jnp.concatenate([eight_rows] * 2, axis=0).astype(jnp.int16)
    rows = lax.broadcasted_iota(jnp.int32, (row_count, 128), 0).astype(jnp.int16)
    spread = jnp.concatenate([sixteen] * (row_count // 16), axis=0)
    rows = jnp.concatenate([rows] * (lanes // 128), axis=1)
    return jnp.where(rows == spread, jnp.bfloat16(1.0), jnp.bfloat16(0.0))


def finish(total, chain, atom, target, w_up, w_atom):
    update = silu(dot_at(total.astype(jnp.bfloat16), w_up, 0, 0))
    edge_out = (chain + update).astype(jnp.bfloat16)
    contrib = matmul(edge_out, w_atom).astype(jnp.bfloat16)
    atom_sum = matmul(hot_columns(atom.shape[0], target), contrib)
    atom_out = (atom.astype(jnp.float32) + silu(0.25 * atom_sum)).astype(jnp.bfloat16)
    return edge_out, atom_out


def block_kernel(n, loaded, *refs):
    sources = refs[:loaded]
    in_hbm, out_hbm, valid_hbm, basis_hbm = refs[loaded : loaded + 4]
    edge_out_ref, atom_out_ref = refs[loaded + 4 : loaded + 6]
    held = refs[loaded + 6 : 2 * loaded + 6]
    (
        stage_v,
        valid_v,
        stage_basis_v,
        ends_out,
        ends_v,
        basis_out,
        basis_v,
        atoms_out,
        atoms_in,
        weight_v,
        chain_v,
        sum_v,
        load_sem,
        stage_sem,
        send_sem,
        recv_sem,
        ready,
    ) = refs[2 * loaded + 6 :]
    (
        atom_v,
        asend_v,
        edge_v,
        w_edge_v,
        source_v,
        w_source_v,
        w_down_v,
        w_bilinear_v,
        w_res_v,
        send_v,
        return_v,
        target_v,
        w_up_v,
        w_atom_v,
    ) = held
    me = lax.axis_index("graph")
    cap = basis_v.shape[2]
    rows = ends_v.shape[1] // 2
    edge_count = edge_v.shape[0]
    width = w_down_v.shape[0]
    basis_count = basis_v.shape[1]
    bf16 = jnp.bfloat16
    layers = ready.shape[0]
    span = n // layers
    layer = lax.div(me, span)
    arrays = (ends_v, basis_v, atoms_in)
    sources_of = (ends_out, basis_out, atoms_out)

    def signal(semaphore, peer):
        pl.semaphore_signal(
            semaphore, inc=1, device_id={"graph": peer}, device_id_type=pl.DeviceIdType.MESH
        )

    barrier = pltpu.get_barrier_semaphore()
    loads = [
        pltpu.make_async_copy(src, dst, load_sem.at[i])
        for i, (src, dst) in enumerate(zip(sources, held))
    ]
    stages = [
        pltpu.make_async_copy(src, dst, stage_sem.at[i])
        for i, (src, dst) in enumerate(
            (
                (in_hbm, stage_v.at[:, pl.ds(0, rows)]),
                (out_hbm, stage_v.at[:, pl.ds(rows, rows)]),
                (valid_hbm, valid_v),
                (basis_hbm, stage_basis_v),
            )
        )
    ]
    for load in loads[:2]:
        load.start()
    for peer in range(n):
        pl.when((layer <= peer // span) & (me != peer))(functools.partial(signal, barrier, peer))
    for stage in stages:
        stage.start()
    for load in loads[2:]:
        load.start()
    pl.semaphore_wait(barrier, span * (layer + 1) - 1)
    for peer in range(n):
        pl.when(layer > peer // span)(functools.partial(signal, ready.at[layer], peer))
    loads[0].wait()
    loads[1].wait()
    picked = dot_at(hot_columns(atom_v.shape[0], asend_v[...]), atom_v[...], 0, 0)
    atoms_out[...] = picked.reshape(atoms_out.shape).astype(bf16)
    def own(kind):
        pltpu.make_async_copy(
            sources_of[kind].at[me], arrays[kind].at[me], recv_sem.at[kind, 0]
        ).start()

    inner = lax.rem(me, span)

    def send(kinds, other):
        apart = partner(layer, other, layers)
        for step in range(span):
            peer = other * span + partner(inner, step, span)

            def start():
                for kind in kinds:
                    pltpu.make_async_remote_copy(
                        src_ref=sources_of[kind].at[peer],
                        dst_ref=arrays[kind].at[me],
                        send_sem=send_sem.at[kind, other],
                        recv_sem=recv_sem.at[kind, 0 if kind == 2 else apart],
                        device_id={"graph": peer},
                        device_id_type=pl.DeviceIdType.MESH,
                    ).start()

            if step:
                start()
            else:
                pl.when(layer != other)(start)

    def sent(kind, other):
        buffer = arrays[kind]

        @pl.when(layer != other)
        def _():
            arrive(buffer.at[pl.ds(0, span)], send_sem.at[kind, other])

        @pl.when(layer == other)
        def _():
            arrive(buffer.at[pl.ds(0, span - 1)], send_sem.at[kind, other])

    def arrive(buffer, sem):
        pltpu.make_async_copy(buffer, buffer, sem).wait()

    own(2)
    for other in range(layers):

        @pl.when(layer >= other)
        def _():
            send((2,), other)

    for stage in stages:
        stage.wait()
    ends_out[...] = stage_v[...].astype(jnp.int16)
    for tile in range(n):
        basis_out[tile] = stage_basis_v[:, tile * cap : (tile + 1) * cap] * valid_v[tile].astype(
            jnp.float32
        ).astype(bf16)
    own(0)
    own(1)
    for other in range(layers):

        @pl.when(layer == other)
        def _():
            send((0, 1), other)

    for other in range(layers):

        @pl.when(layer > other)
        def _():
            send((0, 1), other)

    for load in loads[2:8]:
        load.wait()
    weight_v[...] = jnp.concatenate(
        [w_bilinear_v[:, k * width : (k + 1) * width] for k in range(basis_count)], axis=0
    ).T
    edge = edge_v[...]
    pre_act = matmul(edge, w_edge_v[...])
    pick = hot_columns(atoms_in.shape[0] * atoms_in.shape[1], source_v[...])
    for load in loads[8:]:
        load.wait()
    for other in range(1, layers):

        @pl.when(layer < other)
        def _():
            pl.semaphore_wait(ready.at[other], span)
            send((2,), other)

        @pl.when(layer + 1 == other)
        def _():
            send((0, 1), other)

    for other in range(2, layers):

        @pl.when(layer + 1 < other)
        def _():
            send((0, 1), other)

    arrive(atoms_in, recv_sem.at[2, 0])
    arrived = atoms_in[...].astype(jnp.float32).reshape(pick.shape[0], -1).astype(bf16)
    src_rows = dot_at(pick, arrived, 0, 0).astype(bf16)
    activated = silu(pre_act + matmul(src_rows, w_source_v[...])).astype(bf16)
    projected = silu(dot_at(w_down_v[...], activated, 1, 1)).astype(bf16)
    base = ((edge.astype(jnp.float32) + activated.astype(jnp.float32)) * inv_root).astype(bf16)
    inner_one = silu(matmul(base, w_res_v[0])).astype(bf16)
    middle = ((base.astype(jnp.float32) + silu(matmul(inner_one, w_res_v[1]))) * inv_root).astype(bf16)
    inner_two = silu(matmul(middle, w_res_v[2])).astype(bf16)
    chain_v[...] = (middle.astype(jnp.float32) + silu(matmul(inner_two, w_res_v[3]))) * inv_root

    def gather(tile):
        ends = ends_v[tile].astype(jnp.int32) & (cap - 1)
        in_hot = hot_from(edge_count, look_up(send_v[tile], ends[:rows]))
        gathered = matmul(projected, in_hot).astype(bf16)
        coeffs = basis_v[tile].astype(jnp.float32)
        terms = []
        for k in range(basis_count):
            spread = jnp.broadcast_to(coeffs[k : k + 1, :], (16, cap)).astype(bf16)
            terms.append(jnp.concatenate([spread] * (width // 16), axis=0) * gathered)
        out_hot = hot_from(edge_count, look_up(return_v[tile], ends[rows:]))
        return jnp.concatenate(terms, axis=0), out_hot

    sum_v[...] = jnp.zeros_like(sum_v)

    def some_tiles(group, carry):
        for i in range(APARTS):
            apart = group * APARTS + i
            first = partner(layer, apart, layers) * span
            for kind, buffer in enumerate(arrays[:2]):
                arrive(buffer.at[pl.ds(first, span)], recv_sem.at[kind, apart])
        pairs = [gather(partner(me, group * APARTS * span + i, n)) for i in range(APARTS * span)]
        terms = jnp.concatenate([pair[0] for pair in pairs], axis=1)
        hots = jnp.concatenate([pair[1] for pair in pairs], axis=1)
        sum_v[...] += dot_at(terms, hots, 1, 1)
        return carry

    if UNROLL:
        for group in range(layers // APARTS):
            some_tiles(group, 0)
    else:
        lax.fori_loop(0, layers // APARTS, some_tiles, 0)
    total = matmul(weight_v[...], sum_v[...].astype(bf16))
    edge_out, atom_out = finish(
        total, chain_v[...], atom_v[...], target_v[...], w_up_v[...], w_atom_v[...]
    )
    edge_out_ref[...] = edge_out
    atom_out_ref[...] = atom_out
    for other in range(layers):
        for kind in range(3):
            sent(kind, other)


def on_device(
    n,
    edge_state,
    atom_state,
    atom_sends,
    edge_source,
    edge_target,
    send_edges,
    triplet_in,
    triplet_out,
    triplet_valid,
    triplet_basis,
    return_edges,
    w_edge,
    w_source,
    w_down,
    w_bilinear,
    w_up,
    w_residual,
    w_atom,
):
    cap = triplet_in.shape[0] // n
    layers = 4
    if cap % WIN or cap & (cap - 1) or n & (n - 1) or n < layers:
        return plain_on_device(
            edge_state,
            atom_state,
            atom_sends,
            edge_source,
            edge_target,
            send_edges,
            triplet_in,
            triplet_out,
            triplet_valid,
            triplet_basis,
            return_edges,
            w_edge,
            w_source,
            w_down,
            w_bilinear,
            w_up,
            w_residual,
            w_atom,
        )
    edge_count, edge_width = edge_state.shape
    atom_count, atom_width = atom_state.shape
    basis_count = triplet_basis.shape[0]
    width = w_down.shape[1]
    slots = atom_sends.shape[0] // n
    bf16 = jnp.bfloat16
    loaded = (
        atom_state,
        atom_sends.reshape(1, -1),
        edge_state,
        w_edge,
        edge_source.reshape(1, -1),
        w_source,
        w_down.T,
        w_bilinear,
        w_residual,
        send_edges.reshape(n, 1, cap),
        return_edges.reshape(n, 1, cap),
        edge_target.reshape(1, -1),
        w_up,
        w_atom,
    )
    whole = pl.BlockSpec(memory_space=pltpu.VMEM)
    return pl.pallas_call(
        functools.partial(block_kernel, n, len(loaded)),
        out_shape=(
            pltpu.VMEM((edge_count, edge_width), bf16),
            pltpu.VMEM((atom_count, atom_width), bf16),
        ),
        in_specs=[pl.BlockSpec(memory_space=pl.ANY)] * (len(loaded) + 4),
        out_specs=(whole, whole),
        scratch_shapes=[pltpu.VMEM(each.shape, each.dtype) for each in loaded]
        + [
            pltpu.VMEM((n, 2 * (cap // 128), 128), jnp.int32),
            pltpu.VMEM((n, 1, cap), jnp.int32),
            pltpu.VMEM(triplet_basis.shape, bf16),
            pltpu.VMEM((n, 2 * (cap // 128), 128), jnp.int16),
            pltpu.VMEM((n, 2 * (cap // 128), 128), jnp.int16),
            pltpu.VMEM((n, basis_count, cap), bf16),
            pltpu.VMEM((n, basis_count, cap), bf16),
            pltpu.VMEM((n, slots, atom_width), bf16),
            pltpu.VMEM((n, slots, atom_width), bf16),
            pltpu.VMEM((width, basis_count * width), bf16),
            pltpu.VMEM((edge_count, edge_width), jnp.float32),
            pltpu.VMEM((basis_count * width, edge_count), jnp.float32),
            pltpu.SemaphoreType.DMA((len(loaded),)),
            pltpu.SemaphoreType.DMA((4,)),
            pltpu.SemaphoreType.DMA((3, layers)),
            pltpu.SemaphoreType.DMA((3, layers)),
            pltpu.SemaphoreType.REGULAR((layers,)),
        ],
        compiler_params=pltpu.CompilerParams(collective_id=0, has_side_effects=True),
        name="block",
    )(
        *loaded,
        triplet_in.reshape(n, cap // 128, 128),
        triplet_out.reshape(n, cap // 128, 128),
        triplet_valid.reshape(n, 1, cap),
        triplet_basis,
    )


def solution(mesh):
    placed = (
        P(("groups", "graph"), None),
        P(("groups", "graph"), None),
        P(("groups", "graph")),
        P(("groups", "graph")),
        P(("groups", "graph")),
        P(("groups", "graph")),
        P(("groups", "graph")),
        P(("groups", "graph")),
        P(("groups", "graph")),
        P(None, ("groups", "graph")),
        P(("groups", "graph")),
        P(),
        P(),
        P(),
        P(),
        P(),
        P(),
        P(),
    )
    return jax.shard_map(
        functools.partial(on_device, mesh.shape["graph"]),
        mesh=mesh,
        in_specs=placed,
        out_specs=(P(("groups", "graph"), None), P(("groups", "graph"), None)),
        check_vma=False,
    )
```

```python
import functools

import jax
import jax.numpy as jnp
from jax import lax
from jax.experimental import pallas as pl
from jax.experimental.pallas import tpu as pltpu
from jax.sharding import PartitionSpec as P

WIN = 512
APARTS = 1
UNROLL = False


inv_root = 0.7071067811865476


def matmul(left, right):
    return jnp.dot(left, right, preferred_element_type=jnp.float32)


def pick_rows(indices, table):
    chooser = (indices[:, None] == jnp.arange(table.shape[0], dtype=jnp.int32)[None, :]).astype(
        table.dtype
    )
    return matmul(chooser, table).astype(table.dtype)


def bilinear_terms(inputs_x, coeffs, keeps, w_bilinear):
    expanded = matmul(inputs_x, w_bilinear)
    expanded = expanded.reshape(inputs_x.shape[0], coeffs.shape[0], -1)
    mixed = jnp.einsum("tkd,kt->td", expanded, coeffs.astype(jnp.float32))
    return mixed * keeps.astype(jnp.float32)[:, None]


def tile_sums(slot_rows, local_in, local_out, keeps, coeffs, w_bilinear):
    trip_count = slot_rows.shape[0]
    block_size = WIN
    block_count = trip_count // block_size
    basis_rows = coeffs.shape[0]
    block_iota = jnp.arange(block_size, dtype=jnp.int32)

    def one_block(operands):
        rows_blk, in_blk, out_blk, keep_blk, coef_blk = operands
        in_hot = ((in_blk % block_size)[:, None] == block_iota[None, :]).astype(jnp.bfloat16)
        inputs_x = matmul(in_hot, rows_blk).astype(jnp.bfloat16)
        mixed = bilinear_terms(inputs_x, coef_blk, keep_blk, w_bilinear)
        out_hot = (block_iota[:, None] == (out_blk % block_size)[None, :]).astype(jnp.float32)
        return jnp.dot(
            out_hot, mixed, precision=lax.Precision.HIGHEST, preferred_element_type=jnp.float32
        )

    shaped_coeffs = jnp.transpose(coeffs.reshape(basis_rows, block_count, block_size), (1, 0, 2))
    summed = lax.map(
        one_block,
        (
            slot_rows.reshape(block_count, block_size, -1),
            local_in.reshape(block_count, block_size),
            local_out.reshape(block_count, block_size),
            keeps.reshape(block_count, block_size),
            shaped_coeffs,
        ),
    )
    return summed.reshape(trip_count, -1).astype(jnp.bfloat16)


def plain_on_device(
    edge_state,
    atom_state,
    atom_sends,
    edge_source,
    edge_target,
    send_edges,
    triplet_in,
    triplet_out,
    triplet_valid,
    triplet_basis,
    return_edges,
    w_edge,
    w_source,
    w_down,
    w_bilinear,
    w_up,
    w_residual,
    w_atom,
):
    edge_count = edge_state.shape[0]
    atom_count = atom_state.shape[0]
    arrived_atoms = lax.all_to_all(
        pick_rows(atom_sends, atom_state), "graph", split_axis=0, concat_axis=0, tiled=True
    )
    src_rows = pick_rows(edge_source, arrived_atoms)
    pre_act = matmul(edge_state, w_edge) + matmul(src_rows, w_source)
    activated = jax.nn.silu(pre_act).astype(jnp.bfloat16)
    projected = jax.nn.silu(matmul(activated, w_down)).astype(jnp.bfloat16)
    slot_rows = lax.all_to_all(
        pick_rows(send_edges, projected), "graph", split_axis=0, concat_axis=0, tiled=True
    )
    slot_sums = tile_sums(
        slot_rows, triplet_in, triplet_out, triplet_valid, triplet_basis, w_bilinear
    )
    returned = lax.all_to_all(slot_sums, "graph", split_axis=0, concat_axis=0, tiled=True)
    back_hot = (jnp.arange(edge_count, dtype=jnp.int32)[:, None] == return_edges[None, :]).astype(
        jnp.bfloat16
    )
    aggregate = matmul(back_hot, returned)
    update = jax.nn.silu(matmul(aggregate.astype(jnp.bfloat16), w_up))
    base = ((edge_state.astype(jnp.float32) + activated.astype(jnp.float32)) * inv_root).astype(
        jnp.bfloat16
    )
    inner_one = jax.nn.silu(matmul(base, w_residual[0])).astype(jnp.bfloat16)
    middle = (
        (base.astype(jnp.float32) + jax.nn.silu(matmul(inner_one, w_residual[1]))) * inv_root
    ).astype(jnp.bfloat16)
    inner_two = jax.nn.silu(matmul(middle, w_residual[2])).astype(jnp.bfloat16)
    chain = (middle.astype(jnp.float32) + jax.nn.silu(matmul(inner_two, w_residual[3]))) * inv_root
    edge_out = (chain + update).astype(jnp.bfloat16)
    contrib = matmul(edge_out, w_atom).astype(jnp.bfloat16)
    one_hot = (edge_target[None, :] == jnp.arange(atom_count, dtype=jnp.int32)[:, None]).astype(
        jnp.bfloat16
    )
    atom_sum = matmul(one_hot, contrib)
    atom_out = (atom_state.astype(jnp.float32) + jax.nn.silu(0.25 * atom_sum)).astype(jnp.bfloat16)
    return (edge_out, atom_out)


def silu(value):
    half = 0.5 * value
    return half + half * jnp.tanh(half)


def dot_at(left, right, left_dim, right_dim):
    return lax.dot_general(
        left, right, (((left_dim,), (right_dim,)), ((), ())), preferred_element_type=jnp.float32
    )


def hot_columns(row_count, indices):
    rows = lax.broadcasted_iota(jnp.int32, (row_count, indices.shape[1]), 0)
    return jnp.where(rows == indices, 1.0, 0.0).astype(jnp.bfloat16)


def partner(me, step, n):
    peer = me
    bit = 1
    while bit < n:
        mine = lax.rem(lax.div(me, bit), 2)
        flip = (step // bit) % 2 if isinstance(step, int) else lax.rem(lax.div(step, bit), 2)
        peer = peer + flip * (1 - 2 * mine) * bit
        bit *= 2
    return peer


def look_up(table, indices):
    lanes = indices.shape[1]
    found = []
    for row in range(indices.shape[0]):
        wanted = jnp.broadcast_to(indices[row : row + 1, :], (8, lanes))
        lane = wanted & (lanes - 1)
        value = jnp.zeros_like(wanted)
        for first in range(0, table.shape[1], lanes):
            part = jnp.take_along_axis(
                jnp.broadcast_to(table[:, first : first + lanes], (8, lanes)),
                lane,
                axis=1,
                mode="promise_in_bounds",
            )
            value = jnp.where(wanted - lane == first, part, value)
        found.append(value)
    return jnp.concatenate(found, axis=1)


def hot_from(row_count, eight_rows):
    lanes = eight_rows.shape[1]
    sixteen = jnp.concatenate([eight_rows] * 2, axis=0).astype(jnp.int16)
    rows = lax.broadcasted_iota(jnp.int32, (row_count, 128), 0).astype(jnp.int16)
    spread = jnp.concatenate([sixteen] * (row_count // 16), axis=0)
    rows = jnp.concatenate([rows] * (lanes // 128), axis=1)
    return jnp.where(rows == spread, jnp.bfloat16(1.0), jnp.bfloat16(0.0))


def finish(total, chain, atom, target, w_up, w_atom):
    update = silu(dot_at(total.astype(jnp.bfloat16), w_up, 0, 0))
    edge_out = (chain + update).astype(jnp.bfloat16)
    contrib = matmul(edge_out, w_atom).astype(jnp.bfloat16)
    atom_sum = matmul(hot_columns(atom.shape[0], target), contrib)
    atom_out = (atom.astype(jnp.float32) + silu(0.25 * atom_sum)).astype(jnp.bfloat16)
    return edge_out, atom_out


def block_kernel(n, loaded, *refs):
    sources = refs[:loaded]
    in_hbm, out_hbm, valid_hbm, basis_hbm = refs[loaded : loaded + 4]
    edge_out_ref, atom_out_ref = refs[loaded + 4 : loaded + 6]
    held = refs[loaded + 6 : 2 * loaded + 6]
    (
        stage_v,
        valid_v,
        stage_basis_v,
        ends_out,
        ends_v,
        basis_out,
        basis_v,
        atoms_out,
        atoms_in,
        weight_v,
        chain_v,
        sum_v,
        load_sem,
        stage_sem,
        send_sem,
        recv_sem,
        ready,
    ) = refs[2 * loaded + 6 :]
    (
        atom_v,
        asend_v,
        edge_v,
        w_edge_v,
        source_v,
        w_source_v,
        w_down_v,
        w_bilinear_v,
        w_res_v,
        send_v,
        return_v,
        target_v,
        w_up_v,
        w_atom_v,
    ) = held
    me = lax.axis_index("graph")
    cap = basis_v.shape[2]
    rows = ends_v.shape[1] // 2
    edge_count = edge_v.shape[0]
    width = w_down_v.shape[0]
    basis_count = basis_v.shape[1]
    bf16 = jnp.bfloat16
    layers = ready.shape[0]
    span = n // layers
    layer = lax.div(me, span)
    arrays = (ends_v, basis_v, atoms_in)
    sources_of = (ends_out, basis_out, atoms_out)

    def signal(semaphore, peer):
        pl.semaphore_signal(
            semaphore, inc=1, device_id={"graph": peer}, device_id_type=pl.DeviceIdType.MESH
        )

    barrier = pltpu.get_barrier_semaphore()
    loads = [
        pltpu.make_async_copy(src, dst, load_sem.at[i])
        for i, (src, dst) in enumerate(zip(sources, held))
    ]
    stages = [
        pltpu.make_async_copy(src, dst, stage_sem.at[i])
        for i, (src, dst) in enumerate(
            (
                (in_hbm, stage_v.at[:, pl.ds(0, rows)]),
                (out_hbm, stage_v.at[:, pl.ds(rows, rows)]),
                (valid_hbm, valid_v),
                (basis_hbm, stage_basis_v),
            )
        )
    ]
    for load in loads[:2]:
        load.start()
    for peer in range(n):
        pl.when((layer <= peer // span) & (me != peer))(functools.partial(signal, barrier, peer))
    for stage in stages:
        stage.start()
    for load in loads[2:]:
        load.start()
    pl.semaphore_wait(barrier, span * (layer + 1) - 1)
    for peer in range(n):
        pl.when(layer > peer // span)(functools.partial(signal, ready.at[layer], peer))
    loads[0].wait()
    loads[1].wait()
    picked = dot_at(hot_columns(atom_v.shape[0], asend_v[...]), atom_v[...], 0, 0)
    atoms_out[...] = picked.reshape(atoms_out.shape).astype(bf16)
    def own(kind):
        pltpu.make_async_copy(
            sources_of[kind].at[me], arrays[kind].at[me], recv_sem.at[kind, 0]
        ).start()

    inner = lax.rem(me, span)

    def send(kinds, other):
        apart = partner(layer, other, layers)
        for step in range(span):
            peer = other * span + partner(inner, step, span)

            def start():
                for kind in kinds:
                    pltpu.make_async_remote_copy(
                        src_ref=sources_of[kind].at[peer],
                        dst_ref=arrays[kind].at[me],
                        send_sem=send_sem.at[kind, other],
                        recv_sem=recv_sem.at[kind, 0 if kind == 2 else apart],
                        device_id={"graph": peer},
                        device_id_type=pl.DeviceIdType.MESH,
                    ).start()

            if step:
                start()
            else:
                pl.when(layer != other)(start)

    def sent(kind, other):
        buffer = arrays[kind]

        @pl.when(layer != other)
        def _():
            arrive(buffer.at[pl.ds(0, span)], send_sem.at[kind, other])

        @pl.when(layer == other)
        def _():
            arrive(buffer.at[pl.ds(0, span - 1)], send_sem.at[kind, other])

    def arrive(buffer, sem):
        pltpu.make_async_copy(buffer, buffer, sem).wait()

    own(2)
    for other in range(layers):

        @pl.when(layer >= other)
        def _():
            send((2,), other)

    for stage in stages:
        stage.wait()
    ends_out[...] = stage_v[...].astype(jnp.int16)
    for tile in range(n):
        basis_out[tile] = stage_basis_v[:, tile * cap : (tile + 1) * cap] * valid_v[tile].astype(
            jnp.float32
        ).astype(bf16)
    own(0)
    own(1)
    for other in range(layers):

        @pl.when(layer == other)
        def _():
            send((0, 1), other)

    for other in range(layers):

        @pl.when(layer > other)
        def _():
            send((0, 1), other)

    for load in loads[2:8]:
        load.wait()
    weight_v[...] = jnp.concatenate(
        [w_bilinear_v[:, k * width : (k + 1) * width] for k in range(basis_count)], axis=0
    ).T
    edge = edge_v[...]
    pre_act = matmul(edge, w_edge_v[...])
    pick = hot_columns(atoms_in.shape[0] * atoms_in.shape[1], source_v[...])
    for load in loads[8:]:
        load.wait()
    for other in range(1, layers):

        @pl.when(layer < other)
        def _():
            pl.semaphore_wait(ready.at[other], span)
            send((2,), other)

    for other in range(1, layers):

        @pl.when(layer < other)
        def _():
            send((0, 1), other)

    arrive(atoms_in, recv_sem.at[2, 0])
    arrived = atoms_in[...].astype(jnp.float32).reshape(pick.shape[0], -1).astype(bf16)
    src_rows = dot_at(pick, arrived, 0, 0).astype(bf16)
    activated = silu(pre_act + matmul(src_rows, w_source_v[...])).astype(bf16)
    projected = silu(dot_at(w_down_v[...], activated, 1, 1)).astype(bf16)
    base = ((edge.astype(jnp.float32) + activated.astype(jnp.float32)) * inv_root).astype(bf16)
    inner_one = silu(matmul(base, w_res_v[0])).astype(bf16)
    middle = ((base.astype(jnp.float32) + silu(matmul(inner_one, w_res_v[1]))) * inv_root).astype(bf16)
    inner_two = silu(matmul(middle, w_res_v[2])).astype(bf16)
    chain_v[...] = (middle.astype(jnp.float32) + silu(matmul(inner_two, w_res_v[3]))) * inv_root

    def gather(tile):
        ends = ends_v[tile].astype(jnp.int32) & (cap - 1)
        in_hot = hot_from(edge_count, look_up(send_v[tile], ends[:rows]))
        gathered = matmul(projected, in_hot).astype(bf16)
        coeffs = basis_v[tile].astype(jnp.float32)
        terms = []
        for k in range(basis_count):
            spread = jnp.broadcast_to(coeffs[k : k + 1, :], (16, cap)).astype(bf16)
            terms.append(jnp.concatenate([spread] * (width // 16), axis=0) * gathered)
        out_hot = hot_from(edge_count, look_up(return_v[tile], ends[rows:]))
        return jnp.concatenate(terms, axis=0), out_hot

    sum_v[...] = jnp.zeros_like(sum_v)

    def some_tiles(group, carry):
        for i in range(APARTS):
            apart = group * APARTS + i
            first = partner(layer, apart, layers) * span
            for kind, buffer in enumerate(arrays[:2]):
                arrive(buffer.at[pl.ds(first, span)], recv_sem.at[kind, apart])
        pairs = [gather(partner(me, group * APARTS * span + i, n)) for i in range(APARTS * span)]
        terms = jnp.concatenate([pair[0] for pair in pairs], axis=1)
        hots = jnp.concatenate([pair[1] for pair in pairs], axis=1)
        sum_v[...] += dot_at(terms, hots, 1, 1)
        return carry

    if UNROLL:
        for group in range(layers // APARTS):
            some_tiles(group, 0)
    else:
        lax.fori_loop(0, layers // APARTS, some_tiles, 0)
    total = matmul(weight_v[...], sum_v[...].astype(bf16))
    edge_out, atom_out = finish(
        total, chain_v[...], atom_v[...], target_v[...], w_up_v[...], w_atom_v[...]
    )
    edge_out_ref[...] = edge_out
    atom_out_ref[...] = atom_out
    for other in range(layers):
        for kind in range(3):
            sent(kind, other)


def on_device(
    n,
    edge_state,
    atom_state,
    atom_sends,
    edge_source,
    edge_target,
    send_edges,
    triplet_in,
    triplet_out,
    triplet_valid,
    triplet_basis,
    return_edges,
    w_edge,
    w_source,
    w_down,
    w_bilinear,
    w_up,
    w_residual,
    w_atom,
):
    cap = triplet_in.shape[0] // n
    layers = 4
    if cap % WIN or cap & (cap - 1) or n & (n - 1) or n < layers:
        return plain_on_device(
            edge_state,
            atom_state,
            atom_sends,
            edge_source,
            edge_target,
            send_edges,
            triplet_in,
            triplet_out,
            triplet_valid,
            triplet_basis,
            return_edges,
            w_edge,
            w_source,
            w_down,
            w_bilinear,
            w_up,
            w_residual,
            w_atom,
        )
    edge_count, edge_width = edge_state.shape
    atom_count, atom_width = atom_state.shape
    basis_count = triplet_basis.shape[0]
    width = w_down.shape[1]
    slots = atom_sends.shape[0] // n
    bf16 = jnp.bfloat16
    loaded = (
        atom_state,
        atom_sends.reshape(1, -1),
        edge_state,
        w_edge,
        edge_source.reshape(1, -1),
        w_source,
        w_down.T,
        w_bilinear,
        w_residual,
        send_edges.reshape(n, 1, cap),
        return_edges.reshape(n, 1, cap),
        edge_target.reshape(1, -1),
        w_up,
        w_atom,
    )
    whole = pl.BlockSpec(memory_space=pltpu.VMEM)
    return pl.pallas_call(
        functools.partial(block_kernel, n, len(loaded)),
        out_shape=(
            pltpu.VMEM((edge_count, edge_width), bf16),
            pltpu.VMEM((atom_count, atom_width), bf16),
        ),
        in_specs=[pl.BlockSpec(memory_space=pl.ANY)] * (len(loaded) + 4),
        out_specs=(whole, whole),
        scratch_shapes=[pltpu.VMEM(each.shape, each.dtype) for each in loaded]
        + [
            pltpu.VMEM((n, 2 * (cap // 128), 128), jnp.int32),
            pltpu.VMEM((n, 1, cap), jnp.int32),
            pltpu.VMEM(triplet_basis.shape, bf16),
            pltpu.VMEM((n, 2 * (cap // 128), 128), jnp.int16),
            pltpu.VMEM((n, 2 * (cap // 128), 128), jnp.int16),
            pltpu.VMEM((n, basis_count, cap), bf16),
            pltpu.VMEM((n, basis_count, cap), bf16),
            pltpu.VMEM((n, slots, atom_width), bf16),
            pltpu.VMEM((n, slots, atom_width), bf16),
            pltpu.VMEM((width, basis_count * width), bf16),
            pltpu.VMEM((edge_count, edge_width), jnp.float32),
            pltpu.VMEM((basis_count * width, edge_count), jnp.float32),
            pltpu.SemaphoreType.DMA((len(loaded),)),
            pltpu.SemaphoreType.DMA((4,)),
            pltpu.SemaphoreType.DMA((3, layers)),
            pltpu.SemaphoreType.DMA((3, layers)),
            pltpu.SemaphoreType.REGULAR((layers,)),
        ],
        compiler_params=pltpu.CompilerParams(collective_id=0, has_side_effects=True),
        name="block",
    )(
        *loaded,
        triplet_in.reshape(n, cap // 128, 128),
        triplet_out.reshape(n, cap // 128, 128),
        triplet_valid.reshape(n, 1, cap),
        triplet_basis,
    )


def solution(mesh):
    placed = (
        P(("groups", "graph"), None),
        P(("groups", "graph"), None),
        P(("groups", "graph")),
        P(("groups", "graph")),
        P(("groups", "graph")),
        P(("groups", "graph")),
        P(("groups", "graph")),
        P(("groups", "graph")),
        P(("groups", "graph")),
        P(None, ("groups", "graph")),
        P(("groups", "graph")),
        P(),
        P(),
        P(),
        P(),
        P(),
        P(),
        P(),
    )
    return jax.shard_map(
        functools.partial(on_device, mesh.shape["graph"]),
        mesh=mesh,
        in_specs=placed,
        out_specs=(P(("groups", "graph"), None), P(("groups", "graph"), None)),
        check_vma=False,
    )
```

```python
import functools

import jax
import jax.numpy as jnp
from jax import lax
from jax.experimental import pallas as pl
from jax.experimental.pallas import tpu as pltpu
from jax.sharding import PartitionSpec as P

WIN = 512
APARTS = 1
UNROLL = False


inv_root = 0.7071067811865476


def matmul(left, right):
    return jnp.dot(left, right, preferred_element_type=jnp.float32)


def pick_rows(indices, table):
    chooser = (indices[:, None] == jnp.arange(table.shape[0], dtype=jnp.int32)[None, :]).astype(
        table.dtype
    )
    return matmul(chooser, table).astype(table.dtype)


def bilinear_terms(inputs_x, coeffs, keeps, w_bilinear):
    expanded = matmul(inputs_x, w_bilinear)
    expanded = expanded.reshape(inputs_x.shape[0], coeffs.shape[0], -1)
    mixed = jnp.einsum("tkd,kt->td", expanded, coeffs.astype(jnp.float32))
    return mixed * keeps.astype(jnp.float32)[:, None]


def tile_sums(slot_rows, local_in, local_out, keeps, coeffs, w_bilinear):
    trip_count = slot_rows.shape[0]
    block_size = WIN
    block_count = trip_count // block_size
    basis_rows = coeffs.shape[0]
    block_iota = jnp.arange(block_size, dtype=jnp.int32)

    def one_block(operands):
        rows_blk, in_blk, out_blk, keep_blk, coef_blk = operands
        in_hot = ((in_blk % block_size)[:, None] == block_iota[None, :]).astype(jnp.bfloat16)
        inputs_x = matmul(in_hot, rows_blk).astype(jnp.bfloat16)
        mixed = bilinear_terms(inputs_x, coef_blk, keep_blk, w_bilinear)
        out_hot = (block_iota[:, None] == (out_blk % block_size)[None, :]).astype(jnp.float32)
        return jnp.dot(
            out_hot, mixed, precision=lax.Precision.HIGHEST, preferred_element_type=jnp.float32
        )

    shaped_coeffs = jnp.transpose(coeffs.reshape(basis_rows, block_count, block_size), (1, 0, 2))
    summed = lax.map(
        one_block,
        (
            slot_rows.reshape(block_count, block_size, -1),
            local_in.reshape(block_count, block_size),
            local_out.reshape(block_count, block_size),
            keeps.reshape(block_count, block_size),
            shaped_coeffs,
        ),
    )
    return summed.reshape(trip_count, -1).astype(jnp.bfloat16)


def plain_on_device(
    edge_state,
    atom_state,
    atom_sends,
    edge_source,
    edge_target,
    send_edges,
    triplet_in,
    triplet_out,
    triplet_valid,
    triplet_basis,
    return_edges,
    w_edge,
    w_source,
    w_down,
    w_bilinear,
    w_up,
    w_residual,
    w_atom,
):
    edge_count = edge_state.shape[0]
    atom_count = atom_state.shape[0]
    arrived_atoms = lax.all_to_all(
        pick_rows(atom_sends, atom_state), "graph", split_axis=0, concat_axis=0, tiled=True
    )
    src_rows = pick_rows(edge_source, arrived_atoms)
    pre_act = matmul(edge_state, w_edge) + matmul(src_rows, w_source)
    activated = jax.nn.silu(pre_act).astype(jnp.bfloat16)
    projected = jax.nn.silu(matmul(activated, w_down)).astype(jnp.bfloat16)
    slot_rows = lax.all_to_all(
        pick_rows(send_edges, projected), "graph", split_axis=0, concat_axis=0, tiled=True
    )
    slot_sums = tile_sums(
        slot_rows, triplet_in, triplet_out, triplet_valid, triplet_basis, w_bilinear
    )
    returned = lax.all_to_all(slot_sums, "graph", split_axis=0, concat_axis=0, tiled=True)
    back_hot = (jnp.arange(edge_count, dtype=jnp.int32)[:, None] == return_edges[None, :]).astype(
        jnp.bfloat16
    )
    aggregate = matmul(back_hot, returned)
    update = jax.nn.silu(matmul(aggregate.astype(jnp.bfloat16), w_up))
    base = ((edge_state.astype(jnp.float32) + activated.astype(jnp.float32)) * inv_root).astype(
        jnp.bfloat16
    )
    inner_one = jax.nn.silu(matmul(base, w_residual[0])).astype(jnp.bfloat16)
    middle = (
        (base.astype(jnp.float32) + jax.nn.silu(matmul(inner_one, w_residual[1]))) * inv_root
    ).astype(jnp.bfloat16)
    inner_two = jax.nn.silu(matmul(middle, w_residual[2])).astype(jnp.bfloat16)
    chain = (middle.astype(jnp.float32) + jax.nn.silu(matmul(inner_two, w_residual[3]))) * inv_root
    edge_out = (chain + update).astype(jnp.bfloat16)
    contrib = matmul(edge_out, w_atom).astype(jnp.bfloat16)
    one_hot = (edge_target[None, :] == jnp.arange(atom_count, dtype=jnp.int32)[:, None]).astype(
        jnp.bfloat16
    )
    atom_sum = matmul(one_hot, contrib)
    atom_out = (atom_state.astype(jnp.float32) + jax.nn.silu(0.25 * atom_sum)).astype(jnp.bfloat16)
    return (edge_out, atom_out)


def silu(value):
    half = 0.5 * value
    return half + half * jnp.tanh(half)


def dot_at(left, right, left_dim, right_dim):
    return lax.dot_general(
        left, right, (((left_dim,), (right_dim,)), ((), ())), preferred_element_type=jnp.float32
    )


def hot_columns(row_count, indices):
    rows = lax.broadcasted_iota(jnp.int32, (row_count, indices.shape[1]), 0)
    return jnp.where(rows == indices, 1.0, 0.0).astype(jnp.bfloat16)


def partner(me, step, n):
    peer = me
    bit = 1
    while bit < n:
        mine = lax.rem(lax.div(me, bit), 2)
        flip = (step // bit) % 2 if isinstance(step, int) else lax.rem(lax.div(step, bit), 2)
        peer = peer + flip * (1 - 2 * mine) * bit
        bit *= 2
    return peer


def look_up(table, indices):
    lanes = indices.shape[1]
    found = []
    for row in range(indices.shape[0]):
        wanted = jnp.broadcast_to(indices[row : row + 1, :], (8, lanes))
        lane = wanted & (lanes - 1)
        value = jnp.zeros_like(wanted)
        for first in range(0, table.shape[1], lanes):
            part = jnp.take_along_axis(
                jnp.broadcast_to(table[:, first : first + lanes], (8, lanes)),
                lane,
                axis=1,
                mode="promise_in_bounds",
            )
            value = jnp.where(wanted - lane == first, part, value)
        found.append(value)
    return jnp.concatenate(found, axis=1)


def hot_from(row_count, eight_rows):
    lanes = eight_rows.shape[1]
    sixteen = jnp.concatenate([eight_rows] * 2, axis=0).astype(jnp.int16)
    rows = lax.broadcasted_iota(jnp.int32, (row_count, 128), 0).astype(jnp.int16)
    spread = jnp.concatenate([sixteen] * (row_count // 16), axis=0)
    rows = jnp.concatenate([rows] * (lanes // 128), axis=1)
    return jnp.where(rows == spread, jnp.bfloat16(1.0), jnp.bfloat16(0.0))


def finish(total, chain, atom, target, w_up, w_atom):
    update = silu(dot_at(total.astype(jnp.bfloat16), w_up, 0, 0))
    edge_out = (chain + update).astype(jnp.bfloat16)
    contrib = matmul(edge_out, w_atom).astype(jnp.bfloat16)
    atom_sum = matmul(hot_columns(atom.shape[0], target), contrib)
    atom_out = (atom.astype(jnp.float32) + silu(0.25 * atom_sum)).astype(jnp.bfloat16)
    return edge_out, atom_out


def put_out(edge_v, atom_v, edge_out, atom_out, sem):
    puts = [
        pltpu.make_async_copy(edge_v, edge_out, sem.at[0]),
        pltpu.make_async_copy(atom_v, atom_out, sem.at[1]),
    ]
    for put in puts:
        put.start()
    for put in puts:
        put.wait()


def block_kernel(n, loaded, *refs):
    sources = refs[:loaded]
    in_hbm, out_hbm, valid_hbm, basis_hbm = refs[loaded : loaded + 4]
    edge_out_ref, atom_out_ref = refs[loaded + 4 : loaded + 6]
    held = refs[loaded + 6 : 2 * loaded + 6]
    (
        stage_v,
        valid_v,
        stage_basis_v,
        ends_out,
        ends_v,
        basis_out,
        basis_v,
        atoms_out,
        atoms_in,
        weight_v,
        chain_v,
        sum_v,
        load_sem,
        stage_sem,
        send_sem,
        recv_sem,
        ready,
    ) = refs[2 * loaded + 6 :]
    (
        atom_v,
        asend_v,
        edge_v,
        w_edge_v,
        source_v,
        w_source_v,
        w_down_v,
        w_bilinear_v,
        w_res_v,
        send_v,
        return_v,
        target_v,
        w_up_v,
        w_atom_v,
    ) = held
    me = lax.axis_index("graph")
    cap = basis_v.shape[2]
    rows = ends_v.shape[1] // 2
    edge_count = edge_v.shape[0]
    width = w_down_v.shape[0]
    basis_count = basis_v.shape[1]
    bf16 = jnp.bfloat16
    layers = ready.shape[0]
    span = n // layers
    layer = lax.div(me, span)
    arrays = (ends_v, basis_v, atoms_in)
    sources_of = (ends_out, basis_out, atoms_out)

    def signal(semaphore, peer):
        pl.semaphore_signal(
            semaphore, inc=1, device_id={"graph": peer}, device_id_type=pl.DeviceIdType.MESH
        )

    barrier = pltpu.get_barrier_semaphore()
    loads = [
        pltpu.make_async_copy(src, dst, load_sem.at[i])
        for i, (src, dst) in enumerate(zip(sources, held))
    ]
    stages = [
        pltpu.make_async_copy(src, dst, stage_sem.at[i])
        for i, (src, dst) in enumerate(
            (
                (in_hbm, stage_v.at[:, pl.ds(0, rows)]),
                (out_hbm, stage_v.at[:, pl.ds(rows, rows)]),
                (valid_hbm, valid_v),
                (basis_hbm, stage_basis_v),
            )
        )
    ]
    for load in loads[:2]:
        load.start()
    for peer in range(n):
        pl.when((layer <= peer // span) & (me != peer))(functools.partial(signal, barrier, peer))
    for stage in stages:
        stage.start()
    for load in loads[2:]:
        load.start()
    pl.semaphore_wait(barrier, span * (layer + 1) - 1)
    for peer in range(n):
        pl.when(layer > peer // span)(functools.partial(signal, ready.at[layer], peer))
    loads[0].wait()
    loads[1].wait()
    picked = dot_at(hot_columns(atom_v.shape[0], asend_v[...]), atom_v[...], 0, 0)
    atoms_out[...] = picked.reshape(atoms_out.shape).astype(bf16)
    def own(kind):
        pltpu.make_async_copy(
            sources_of[kind].at[me], arrays[kind].at[me], recv_sem.at[kind, 0]
        ).start()

    inner = lax.rem(me, span)

    def send(kinds, other):
        apart = partner(layer, other, layers)
        for step in range(span):
            peer = other * span + partner(inner, step, span)

            def start():
                for kind in kinds:
                    pltpu.make_async_remote_copy(
                        src_ref=sources_of[kind].at[peer],
                        dst_ref=arrays[kind].at[me],
                        send_sem=send_sem.at[kind, other],
                        recv_sem=recv_sem.at[kind, 0 if kind == 2 else apart],
                        device_id={"graph": peer},
                        device_id_type=pl.DeviceIdType.MESH,
                    ).start()

            if step:
                start()
            else:
                pl.when(layer != other)(start)

    def sent(kind, other):
        buffer = arrays[kind]

        @pl.when(layer != other)
        def _():
            arrive(buffer.at[pl.ds(0, span)], send_sem.at[kind, other])

        @pl.when(layer == other)
        def _():
            arrive(buffer.at[pl.ds(0, span - 1)], send_sem.at[kind, other])

    def arrive(buffer, sem):
        pltpu.make_async_copy(buffer, buffer, sem).wait()

    own(2)
    for other in range(layers):

        @pl.when(layer >= other)
        def _():
            send((2,), other)

    for stage in stages:
        stage.wait()
    ends_out[...] = stage_v[...].astype(jnp.int16)
    for tile in range(n):
        basis_out[tile] = stage_basis_v[:, tile * cap : (tile + 1) * cap] * valid_v[tile].astype(
            jnp.float32
        ).astype(bf16)
    own(0)
    own(1)
    for other in range(layers):

        @pl.when(layer == other)
        def _():
            send((0, 1), other)

    for other in range(layers):

        @pl.when(layer > other)
        def _():
            send((0, 1), other)

    for load in loads[2:8]:
        load.wait()
    weight_v[...] = jnp.concatenate(
        [w_bilinear_v[:, k * width : (k + 1) * width] for k in range(basis_count)], axis=0
    ).T
    edge = edge_v[...]
    pre_act = matmul(edge, w_edge_v[...])
    pick = hot_columns(atoms_in.shape[0] * atoms_in.shape[1], source_v[...])
    for load in loads[8:]:
        load.wait()
    for other in range(1, layers):

        @pl.when(layer < other)
        def _():
            pl.semaphore_wait(ready.at[other], span)
            send((2,), other)

    for other in range(1, layers):

        @pl.when(layer < other)
        def _():
            send((0, 1), other)

    arrive(atoms_in, recv_sem.at[2, 0])
    arrived = atoms_in[...].astype(jnp.float32).reshape(pick.shape[0], -1).astype(bf16)
    src_rows = dot_at(pick, arrived, 0, 0).astype(bf16)
    activated = silu(pre_act + matmul(src_rows, w_source_v[...])).astype(bf16)
    projected = silu(dot_at(w_down_v[...], activated, 1, 1)).astype(bf16)
    base = ((edge.astype(jnp.float32) + activated.astype(jnp.float32)) * inv_root).astype(bf16)
    inner_one = silu(matmul(base, w_res_v[0])).astype(bf16)
    middle = ((base.astype(jnp.float32) + silu(matmul(inner_one, w_res_v[1]))) * inv_root).astype(bf16)
    inner_two = silu(matmul(middle, w_res_v[2])).astype(bf16)
    chain_v[...] = (middle.astype(jnp.float32) + silu(matmul(inner_two, w_res_v[3]))) * inv_root

    def gather(tile):
        ends = ends_v[tile].astype(jnp.int32) & (cap - 1)
        in_hot = hot_from(edge_count, look_up(send_v[tile], ends[:rows]))
        gathered = matmul(projected, in_hot).astype(bf16)
        coeffs = basis_v[tile].astype(jnp.float32)
        terms = []
        for k in range(basis_count):
            spread = jnp.broadcast_to(coeffs[k : k + 1, :], (16, cap)).astype(bf16)
            terms.append(jnp.concatenate([spread] * (width // 16), axis=0) * gathered)
        out_hot = hot_from(edge_count, look_up(return_v[tile], ends[rows:]))
        return jnp.concatenate(terms, axis=0), out_hot

    sum_v[...] = jnp.zeros_like(sum_v)

    def some_tiles(group, carry):
        for i in range(APARTS):
            apart = group * APARTS + i
            first = partner(layer, apart, layers) * span
            for kind, buffer in enumerate(arrays[:2]):
                arrive(buffer.at[pl.ds(first, span)], recv_sem.at[kind, apart])
        pairs = [gather(partner(me, group * APARTS * span + i, n)) for i in range(APARTS * span)]
        terms = jnp.concatenate([pair[0] for pair in pairs], axis=1)
        hots = jnp.concatenate([pair[1] for pair in pairs], axis=1)
        sum_v[...] += dot_at(terms, hots, 1, 1)
        return carry

    if UNROLL:
        for group in range(layers // APARTS):
            some_tiles(group, 0)
    else:
        lax.fori_loop(0, layers // APARTS, some_tiles, 0)
    total = matmul(weight_v[...], sum_v[...].astype(bf16))
    edge_out, atom_out = finish(
        total, chain_v[...], atom_v[...], target_v[...], w_up_v[...], w_atom_v[...]
    )
    edge_out_ref[...] = edge_out
    atom_out_ref[...] = atom_out
    for other in range(layers):
        for kind in range(3):
            sent(kind, other)


def on_device(
    n,
    edge_state,
    atom_state,
    atom_sends,
    edge_source,
    edge_target,
    send_edges,
    triplet_in,
    triplet_out,
    triplet_valid,
    triplet_basis,
    return_edges,
    w_edge,
    w_source,
    w_down,
    w_bilinear,
    w_up,
    w_residual,
    w_atom,
):
    cap = triplet_in.shape[0] // n
    layers = 4
    if cap % WIN or cap & (cap - 1) or n & (n - 1) or n < layers:
        return plain_on_device(
            edge_state,
            atom_state,
            atom_sends,
            edge_source,
            edge_target,
            send_edges,
            triplet_in,
            triplet_out,
            triplet_valid,
            triplet_basis,
            return_edges,
            w_edge,
            w_source,
            w_down,
            w_bilinear,
            w_up,
            w_residual,
            w_atom,
        )
    edge_count, edge_width = edge_state.shape
    atom_count, atom_width = atom_state.shape
    basis_count = triplet_basis.shape[0]
    width = w_down.shape[1]
    slots = atom_sends.shape[0] // n
    bf16 = jnp.bfloat16
    loaded = (
        atom_state,
        atom_sends.reshape(1, -1),
        edge_state,
        w_edge,
        edge_source.reshape(1, -1),
        w_source,
        w_down.T,
        w_bilinear,
        w_residual,
        send_edges.reshape(n, 1, cap),
        return_edges.reshape(n, 1, cap),
        edge_target.reshape(1, -1),
        w_up,
        w_atom,
    )
    whole = pl.BlockSpec(memory_space=pltpu.VMEM)
    edge_out, atom_out = pl.pallas_call(
        functools.partial(block_kernel, n, len(loaded)),
        out_shape=(
            pltpu.VMEM((edge_count, edge_width), bf16),
            pltpu.VMEM((atom_count, atom_width), bf16),
        ),
        in_specs=[pl.BlockSpec(memory_space=pl.ANY)] * (len(loaded) + 4),
        out_specs=(whole, whole),
        scratch_shapes=[pltpu.VMEM(each.shape, each.dtype) for each in loaded]
        + [
            pltpu.VMEM((n, 2 * (cap // 128), 128), jnp.int32),
            pltpu.VMEM((n, 1, cap), jnp.int32),
            pltpu.VMEM(triplet_basis.shape, bf16),
            pltpu.VMEM((n, 2 * (cap // 128), 128), jnp.int16),
            pltpu.VMEM((n, 2 * (cap // 128), 128), jnp.int16),
            pltpu.VMEM((n, basis_count, cap), bf16),
            pltpu.VMEM((n, basis_count, cap), bf16),
            pltpu.VMEM((n, slots, atom_width), bf16),
            pltpu.VMEM((n, slots, atom_width), bf16),
            pltpu.VMEM((width, basis_count * width), bf16),
            pltpu.VMEM((edge_count, edge_width), jnp.float32),
            pltpu.VMEM((basis_count * width, edge_count), jnp.float32),
            pltpu.SemaphoreType.DMA((len(loaded),)),
            pltpu.SemaphoreType.DMA((4,)),
            pltpu.SemaphoreType.DMA((3, layers)),
            pltpu.SemaphoreType.DMA((3, layers)),
            pltpu.SemaphoreType.REGULAR((layers,)),
        ],
        compiler_params=pltpu.CompilerParams(collective_id=0, has_side_effects=True),
        name="block",
    )(
        *loaded,
        triplet_in.reshape(n, cap // 128, 128),
        triplet_out.reshape(n, cap // 128, 128),
        triplet_valid.reshape(n, 1, cap),
        triplet_basis,
    )
    return pl.pallas_call(
        put_out,
        out_shape=(
            jax.ShapeDtypeStruct(edge_out.shape, bf16),
            jax.ShapeDtypeStruct(atom_out.shape, bf16),
        ),
        in_specs=[whole, whole],
        out_specs=(pl.BlockSpec(memory_space=pl.ANY),) * 2,
        scratch_shapes=[pltpu.SemaphoreType.DMA((2,))],
        name="tail",
    )(
        pltpu.with_memory_space_constraint(edge_out, pltpu.VMEM),
        pltpu.with_memory_space_constraint(atom_out, pltpu.VMEM),
    )


def solution(mesh):
    placed = (
        P(("groups", "graph"), None),
        P(("groups", "graph"), None),
        P(("groups", "graph")),
        P(("groups", "graph")),
        P(("groups", "graph")),
        P(("groups", "graph")),
        P(("groups", "graph")),
        P(("groups", "graph")),
        P(("groups", "graph")),
        P(None, ("groups", "graph")),
        P(("groups", "graph")),
        P(),
        P(),
        P(),
        P(),
        P(),
        P(),
        P(),
    )
    return jax.shard_map(
        functools.partial(on_device, mesh.shape["graph"]),
        mesh=mesh,
        in_specs=placed,
        out_specs=(P(("groups", "graph"), None), P(("groups", "graph"), None)),
        check_vma=False,
    )
```

```python
import functools

import jax
import jax.numpy as jnp
from jax import lax
from jax.experimental import pallas as pl
from jax.experimental.pallas import tpu as pltpu
from jax.sharding import PartitionSpec as P

WIN = 512
HALVES = 2


inv_root = 0.7071067811865476


def matmul(left, right):
    return jnp.dot(left, right, preferred_element_type=jnp.float32)


def pick_rows(indices, table):
    chooser = (indices[:, None] == jnp.arange(table.shape[0], dtype=jnp.int32)[None, :]).astype(
        table.dtype
    )
    return matmul(chooser, table).astype(table.dtype)


def bilinear_terms(inputs_x, coeffs, keeps, w_bilinear):
    expanded = matmul(inputs_x, w_bilinear)
    expanded = expanded.reshape(inputs_x.shape[0], coeffs.shape[0], -1)
    mixed = jnp.einsum("tkd,kt->td", expanded, coeffs.astype(jnp.float32))
    return mixed * keeps.astype(jnp.float32)[:, None]


def tile_sums(slot_rows, local_in, local_out, keeps, coeffs, w_bilinear):
    trip_count = slot_rows.shape[0]
    block_size = WIN
    block_count = trip_count // block_size
    basis_rows = coeffs.shape[0]
    block_iota = jnp.arange(block_size, dtype=jnp.int32)

    def one_block(operands):
        rows_blk, in_blk, out_blk, keep_blk, coef_blk = operands
        in_hot = ((in_blk % block_size)[:, None] == block_iota[None, :]).astype(jnp.bfloat16)
        inputs_x = matmul(in_hot, rows_blk).astype(jnp.bfloat16)
        mixed = bilinear_terms(inputs_x, coef_blk, keep_blk, w_bilinear)
        out_hot = (block_iota[:, None] == (out_blk % block_size)[None, :]).astype(jnp.float32)
        return jnp.dot(
            out_hot, mixed, precision=lax.Precision.HIGHEST, preferred_element_type=jnp.float32
        )

    shaped_coeffs = jnp.transpose(coeffs.reshape(basis_rows, block_count, block_size), (1, 0, 2))
    summed = lax.map(
        one_block,
        (
            slot_rows.reshape(block_count, block_size, -1),
            local_in.reshape(block_count, block_size),
            local_out.reshape(block_count, block_size),
            keeps.reshape(block_count, block_size),
            shaped_coeffs,
        ),
    )
    return summed.reshape(trip_count, -1).astype(jnp.bfloat16)


def plain_on_device(
    edge_state,
    atom_state,
    atom_sends,
    edge_source,
    edge_target,
    send_edges,
    triplet_in,
    triplet_out,
    triplet_valid,
    triplet_basis,
    return_edges,
    w_edge,
    w_source,
    w_down,
    w_bilinear,
    w_up,
    w_residual,
    w_atom,
):
    edge_count = edge_state.shape[0]
    atom_count = atom_state.shape[0]
    arrived_atoms = lax.all_to_all(
        pick_rows(atom_sends, atom_state), "graph", split_axis=0, concat_axis=0, tiled=True
    )
    src_rows = pick_rows(edge_source, arrived_atoms)
    pre_act = matmul(edge_state, w_edge) + matmul(src_rows, w_source)
    activated = jax.nn.silu(pre_act).astype(jnp.bfloat16)
    projected = jax.nn.silu(matmul(activated, w_down)).astype(jnp.bfloat16)
    slot_rows = lax.all_to_all(
        pick_rows(send_edges, projected), "graph", split_axis=0, concat_axis=0, tiled=True
    )
    slot_sums = tile_sums(
        slot_rows, triplet_in, triplet_out, triplet_valid, triplet_basis, w_bilinear
    )
    returned = lax.all_to_all(slot_sums, "graph", split_axis=0, concat_axis=0, tiled=True)
    back_hot = (jnp.arange(edge_count, dtype=jnp.int32)[:, None] == return_edges[None, :]).astype(
        jnp.bfloat16
    )
    aggregate = matmul(back_hot, returned)
    update = jax.nn.silu(matmul(aggregate.astype(jnp.bfloat16), w_up))
    base = ((edge_state.astype(jnp.float32) + activated.astype(jnp.float32)) * inv_root).astype(
        jnp.bfloat16
    )
    inner_one = jax.nn.silu(matmul(base, w_residual[0])).astype(jnp.bfloat16)
    middle = (
        (base.astype(jnp.float32) + jax.nn.silu(matmul(inner_one, w_residual[1]))) * inv_root
    ).astype(jnp.bfloat16)
    inner_two = jax.nn.silu(matmul(middle, w_residual[2])).astype(jnp.bfloat16)
    chain = (middle.astype(jnp.float32) + jax.nn.silu(matmul(inner_two, w_residual[3]))) * inv_root
    edge_out = (chain + update).astype(jnp.bfloat16)
    contrib = matmul(edge_out, w_atom).astype(jnp.bfloat16)
    one_hot = (edge_target[None, :] == jnp.arange(atom_count, dtype=jnp.int32)[:, None]).astype(
        jnp.bfloat16
    )
    atom_sum = matmul(one_hot, contrib)
    atom_out = (atom_state.astype(jnp.float32) + jax.nn.silu(0.25 * atom_sum)).astype(jnp.bfloat16)
    return (edge_out, atom_out)


def silu(value):
    half = 0.5 * value
    return half + half * jnp.tanh(half)


def dot_at(left, right, left_dim, right_dim):
    return lax.dot_general(
        left, right, (((left_dim,), (right_dim,)), ((), ())), preferred_element_type=jnp.float32
    )


def hot_columns(row_count, indices):
    rows = lax.broadcasted_iota(jnp.int32, (row_count, indices.shape[1]), 0)
    return jnp.where(rows == indices, 1.0, 0.0).astype(jnp.bfloat16)


def partner(me, step, n):
    peer = me
    bit = 1
    while bit < n:
        mine = lax.rem(lax.div(me, bit), 2)
        flip = (step // bit) % 2 if isinstance(step, int) else lax.rem(lax.div(step, bit), 2)
        peer = peer + flip * (1 - 2 * mine) * bit
        bit *= 2
    return peer


def look_up(table, indices):
    lanes = indices.shape[1]
    found = []
    for row in range(indices.shape[0]):
        wanted = jnp.broadcast_to(indices[row : row + 1, :], (8, lanes))
        lane = wanted & (lanes - 1)
        value = jnp.zeros_like(wanted)
        for first in range(0, table.shape[1], lanes):
            part = jnp.take_along_axis(
                jnp.broadcast_to(table[:, first : first + lanes], (8, lanes)),
                lane,
                axis=1,
                mode="promise_in_bounds",
            )
            value = jnp.where(wanted - lane == first, part, value)
        found.append(value)
    return jnp.concatenate(found, axis=1)


def pick_columns(table, indices):
    lanes = 128
    found = []
    for start in range(0, indices.shape[1], lanes):
        wanted = indices[:, start : start + lanes]
        lane = wanted & (lanes - 1)
        blocks = []
        for row in range(0, table.shape[0], 8):
            value = None
            for first in range(0, table.shape[1], lanes):
                part = jnp.take_along_axis(
                    table[row : row + 8, first : first + lanes],
                    lane,
                    axis=1,
                    mode="promise_in_bounds",
                )
                value = part if value is None else jnp.where(wanted - lane == first, part, value)
            blocks.append(value)
        found.append(jnp.concatenate(blocks, axis=0))
    return jnp.concatenate(found, axis=1)


def hot_from(row_count, eight_rows):
    lanes = eight_rows.shape[1]
    sixteen = jnp.concatenate([eight_rows] * 2, axis=0).astype(jnp.int16)
    rows = lax.broadcasted_iota(jnp.int32, (row_count, 128), 0).astype(jnp.int16)
    spread = jnp.concatenate([sixteen] * (row_count // 16), axis=0)
    rows = jnp.concatenate([rows] * (lanes // 128), axis=1)
    return jnp.where(rows == spread, jnp.bfloat16(1.0), jnp.bfloat16(0.0))


def finish(total, chain, atom, target, w_up, w_atom):
    update = silu(dot_at(total.astype(jnp.bfloat16), w_up, 0, 0))
    edge_out = (chain + update).astype(jnp.bfloat16)
    contrib = matmul(edge_out, w_atom).astype(jnp.bfloat16)
    atom_sum = matmul(hot_columns(atom.shape[0], target), contrib)
    atom_out = (atom.astype(jnp.float32) + silu(0.25 * atom_sum)).astype(jnp.bfloat16)
    return edge_out, atom_out


def put_out(edge_v, atom_v, edge_out, atom_out, sem):
    puts = [
        pltpu.make_async_copy(edge_v, edge_out, sem.at[0]),
        pltpu.make_async_copy(atom_v, atom_out, sem.at[1]),
    ]
    for put in puts:
        put.start()
    for put in puts:
        put.wait()


def block_kernel(n, loaded, *refs):
    sources = refs[:loaded]
    in_hbm, out_hbm, valid_hbm, basis_hbm = refs[loaded : loaded + 4]
    edge_out_ref, atom_out_ref = refs[loaded + 4 : loaded + 6]
    held = refs[loaded + 6 : 2 * loaded + 6]
    (
        stage_v,
        valid_v,
        stage_basis_v,
        ends_out,
        ends_v,
        basis_out,
        basis_v,
        atoms_out,
        atoms_in,
        weight_v,
        rows_even,
        rows_odd,
        hots_even,
        hots_odd,
        chain_v,
        sum_v,
        load_sem,
        stage_sem,
        send_sem,
        recv_sem,
        ready,
    ) = refs[2 * loaded + 6 :]
    (
        atom_v,
        asend_v,
        edge_v,
        w_edge_v,
        source_v,
        w_source_v,
        w_down_v,
        w_bilinear_v,
        w_res_v,
        send_v,
        return_v,
        target_v,
        w_up_v,
        w_atom_v,
    ) = held
    me = lax.axis_index("graph")
    cap = basis_v.shape[2]
    rows = ends_v.shape[1] // 2
    edge_count = edge_v.shape[0]
    width = w_down_v.shape[0]
    basis_count = basis_v.shape[1]
    bf16 = jnp.bfloat16
    layers = ready.shape[0]
    span = n // layers
    layer = lax.div(me, span)
    rows_v = (rows_even, rows_odd)
    hots_v = (hots_even, hots_odd)
    arrays = (ends_v, basis_v, atoms_in)
    sources_of = (ends_out, basis_out, atoms_out)

    def signal(semaphore, peer):
        pl.semaphore_signal(
            semaphore, inc=1, device_id={"graph": peer}, device_id_type=pl.DeviceIdType.MESH
        )

    barrier = pltpu.get_barrier_semaphore()
    loads = [
        pltpu.make_async_copy(src, dst, load_sem.at[i])
        for i, (src, dst) in enumerate(zip(sources, held))
    ]
    stages = [
        pltpu.make_async_copy(src, dst, stage_sem.at[i])
        for i, (src, dst) in enumerate(
            (
                (in_hbm, stage_v.at[:, pl.ds(0, rows)]),
                (out_hbm, stage_v.at[:, pl.ds(rows, rows)]),
                (valid_hbm, valid_v),
                (basis_hbm, stage_basis_v),
            )
        )
    ]
    for load in loads[:2]:
        load.start()
    for stage in stages:
        stage.start()
    for peer in range(n):
        pl.when((layer <= peer // span) & (me != peer))(functools.partial(signal, barrier, peer))
    for load in loads[2:]:
        load.start()
    pl.semaphore_wait(barrier, span * (layer + 1) - 1)
    for peer in range(n):
        pl.when(layer > peer // span)(functools.partial(signal, ready.at[layer], peer))
    loads[0].wait()
    loads[1].wait()
    picked = dot_at(hot_columns(atom_v.shape[0], asend_v[...]), atom_v[...], 0, 0)
    atoms_out[...] = picked.reshape(atoms_out.shape).astype(bf16)
    def own(kind):
        pltpu.make_async_copy(
            sources_of[kind].at[me], arrays[kind].at[me], recv_sem.at[kind, 0]
        ).start()

    inner = lax.rem(me, span)

    def send(kinds, other):
        apart = partner(layer, other, layers)
        for step in range(span):
            peer = other * span + partner(inner, step, span)

            def start():
                for kind in kinds:
                    pltpu.make_async_remote_copy(
                        src_ref=sources_of[kind].at[peer],
                        dst_ref=arrays[kind].at[me],
                        send_sem=send_sem.at[kind],
                        recv_sem=recv_sem.at[kind, 0 if kind == 2 else apart],
                        device_id={"graph": peer},
                        device_id_type=pl.DeviceIdType.MESH,
                    ).start()

            if step:
                start()
            else:
                pl.when(layer != other)(start)

    def arrive(buffer, sem):
        pltpu.make_async_copy(buffer, buffer, sem).wait()

    own(2)
    for other in range(layers):

        @pl.when(layer >= other)
        def _():
            send((2,), other)

    for stage in stages:
        stage.wait()
    ends_out[...] = stage_v[...].astype(jnp.int16)
    for tile in range(n):
        basis_out[tile] = stage_basis_v[:, tile * cap : (tile + 1) * cap] * valid_v[tile].astype(
            jnp.float32
        ).astype(bf16)
    own(0)
    own(1)
    for other in range(layers):

        @pl.when(layer == other)
        def _():
            send((0, 1), other)

    for other in range(layers):

        @pl.when(layer > other)
        def _():
            send((0, 1), other)

    for load in loads[2:8]:
        load.wait()
    weight_v[...] = jnp.concatenate(
        [w_bilinear_v[:, k * width : (k + 1) * width] for k in range(basis_count)], axis=0
    ).T
    edge = edge_v[...]
    pre_act = matmul(edge, w_edge_v[...])
    pick = hot_columns(atoms_in.shape[0] * atoms_in.shape[1], source_v[...])
    for load in loads[8:]:
        load.wait()
    for other in range(1, layers):

        @pl.when(layer < other)
        def _():
            pl.semaphore_wait(ready.at[other], span)
            send((2,), other)

    for other in range(1, layers):

        @pl.when(layer < other)
        def _():
            send((0, 1), other)

    arrive(atoms_in, recv_sem.at[2, 0])
    for kind, buffer in enumerate(arrays[:2]):
        arrive(buffer.at[pl.ds(layer * span, span)], recv_sem.at[kind, 0])
    arrived = atoms_in[...].astype(jnp.float32).reshape(pick.shape[0], -1).astype(bf16)
    src_rows = dot_at(pick, arrived, 0, 0).astype(bf16)
    activated = silu(pre_act + matmul(src_rows, w_source_v[...])).astype(bf16)
    projected = silu(dot_at(w_down_v[...], activated, 1, 1)).astype(bf16)
    base = ((edge.astype(jnp.float32) + activated.astype(jnp.float32)) * inv_root).astype(bf16)
    inner_one = silu(matmul(base, w_res_v[0])).astype(bf16)
    middle = ((base.astype(jnp.float32) + silu(matmul(inner_one, w_res_v[1]))) * inv_root).astype(bf16)
    inner_two = silu(matmul(middle, w_res_v[2])).astype(bf16)
    chain_v[...] = (middle.astype(jnp.float32) + silu(matmul(inner_two, w_res_v[3]))) * inv_root

    def first_of(apart):
        return partner(layer, apart, layers) * span

    def prepare(apart):
        for i in range(span):
            tile = first_of(apart) + i
            ends = ends_v[tile].astype(jnp.int32) & (cap - 1)
            edges = look_up(send_v[tile], ends[:rows])
            rows_v[apart % 2][i] = pick_columns(projected.astype(jnp.float32), edges).astype(bf16)
            targets = look_up(return_v[tile], ends[rows:])
            hots_v[apart % 2][i] = hot_from(edge_count, targets)

    def add_terms(apart):
        share = basis_count // HALVES
        hots = jnp.concatenate([hots_v[apart % 2][i] for i in range(span)], axis=1)
        for half in range(HALVES):
            all_terms = []
            for i in range(span):
                gathered = rows_v[apart % 2][i]
                coeffs = basis_v[first_of(apart) + i].astype(jnp.float32)
                terms = []
                for k in range(half * share, (half + 1) * share):
                    spread = jnp.broadcast_to(coeffs[k : k + 1, :], (16, cap)).astype(bf16)
                    terms.append(jnp.concatenate([spread] * (width // 16), axis=0) * gathered)
                all_terms.append(jnp.concatenate(terms, axis=0))
            part = dot_at(jnp.concatenate(all_terms, axis=1), hots, 1, 1)
            slots = pl.ds(half * share * width, share * width)
            if apart:
                sum_v[slots, :] += part
            else:
                sum_v[slots, :] = part

    def arrived_from(apart):
        for kind, buffer in enumerate(arrays[:2]):
            arrive(buffer.at[pl.ds(first_of(apart), span)], recv_sem.at[kind, apart])

    prepare(0)
    for apart in range(layers):
        add_terms(apart)
        if apart + 1 < layers:
            arrived_from(apart + 1)
            prepare(apart + 1)
    total = matmul(weight_v[...], sum_v[...].astype(bf16))
    edge_out, atom_out = finish(
        total, chain_v[...], atom_v[...], target_v[...], w_up_v[...], w_atom_v[...]
    )
    edge_out_ref[...] = edge_out
    atom_out_ref[...] = atom_out
    for kind, buffer in enumerate(arrays):
        arrive(buffer.at[pl.ds(0, n - 1)], send_sem.at[kind])


def on_device(
    n,
    edge_state,
    atom_state,
    atom_sends,
    edge_source,
    edge_target,
    send_edges,
    triplet_in,
    triplet_out,
    triplet_valid,
    triplet_basis,
    return_edges,
    w_edge,
    w_source,
    w_down,
    w_bilinear,
    w_up,
    w_residual,
    w_atom,
):
    cap = triplet_in.shape[0] // n
    layers = 4
    if cap % WIN or cap & (cap - 1) or n & (n - 1) or n < layers:
        return plain_on_device(
            edge_state,
            atom_state,
            atom_sends,
            edge_source,
            edge_target,
            send_edges,
            triplet_in,
            triplet_out,
            triplet_valid,
            triplet_basis,
            return_edges,
            w_edge,
            w_source,
            w_down,
            w_bilinear,
            w_up,
            w_residual,
            w_atom,
        )
    edge_count, edge_width = edge_state.shape
    atom_count, atom_width = atom_state.shape
    basis_count = triplet_basis.shape[0]
    width = w_down.shape[1]
    slots = atom_sends.shape[0] // n
    bf16 = jnp.bfloat16
    loaded = (
        atom_state,
        atom_sends.reshape(1, -1),
        edge_state,
        w_edge,
        edge_source.reshape(1, -1),
        w_source,
        w_down.T,
        w_bilinear,
        w_residual,
        send_edges.reshape(n, 1, cap),
        return_edges.reshape(n, 1, cap),
        edge_target.reshape(1, -1),
        w_up,
        w_atom,
    )
    whole = pl.BlockSpec(memory_space=pltpu.VMEM)
    edge_out, atom_out = pl.pallas_call(
        functools.partial(block_kernel, n, len(loaded)),
        out_shape=(
            pltpu.VMEM((edge_count, edge_width), bf16),
            pltpu.VMEM((atom_count, atom_width), bf16),
        ),
        in_specs=[pl.BlockSpec(memory_space=pl.ANY)] * (len(loaded) + 4),
        out_specs=(whole, whole),
        scratch_shapes=[pltpu.VMEM(each.shape, each.dtype) for each in loaded]
        + [
            pltpu.VMEM((n, 2 * (cap // 128), 128), jnp.int32),
            pltpu.VMEM((n, 1, cap), jnp.int32),
            pltpu.VMEM(triplet_basis.shape, bf16),
            pltpu.VMEM((n, 2 * (cap // 128), 128), jnp.int16),
            pltpu.VMEM((n, 2 * (cap // 128), 128), jnp.int16),
            pltpu.VMEM((n, basis_count, cap), bf16),
            pltpu.VMEM((n, basis_count, cap), bf16),
            pltpu.VMEM((n, slots, atom_width), bf16),
            pltpu.VMEM((n, slots, atom_width), bf16),
            pltpu.VMEM((width, basis_count * width), bf16),
            pltpu.VMEM((n // layers, width, cap), bf16),
            pltpu.VMEM((n // layers, width, cap), bf16),
            pltpu.VMEM((n // layers, edge_count, cap), bf16),
            pltpu.VMEM((n // layers, edge_count, cap), bf16),
            pltpu.VMEM((edge_count, edge_width), jnp.float32),
            pltpu.VMEM((basis_count * width, edge_count), jnp.float32),
            pltpu.SemaphoreType.DMA((len(loaded),)),
            pltpu.SemaphoreType.DMA((4,)),
            pltpu.SemaphoreType.DMA((3,)),
            pltpu.SemaphoreType.DMA((3, layers)),
            pltpu.SemaphoreType.REGULAR((layers,)),
        ],
        compiler_params=pltpu.CompilerParams(collective_id=0, has_side_effects=True),
        name="block",
    )(
        *loaded,
        triplet_in.reshape(n, cap // 128, 128),
        triplet_out.reshape(n, cap // 128, 128),
        triplet_valid.reshape(n, 1, cap),
        triplet_basis,
    )
    return pl.pallas_call(
        put_out,
        out_shape=(
            jax.ShapeDtypeStruct(edge_out.shape, bf16),
            jax.ShapeDtypeStruct(atom_out.shape, bf16),
        ),
        in_specs=[whole, whole],
        out_specs=(pl.BlockSpec(memory_space=pl.ANY),) * 2,
        scratch_shapes=[pltpu.SemaphoreType.DMA((2,))],
        name="tail",
    )(
        pltpu.with_memory_space_constraint(edge_out, pltpu.VMEM),
        pltpu.with_memory_space_constraint(atom_out, pltpu.VMEM),
    )


def solution(mesh):
    placed = (
        P(("groups", "graph"), None),
        P(("groups", "graph"), None),
        P(("groups", "graph")),
        P(("groups", "graph")),
        P(("groups", "graph")),
        P(("groups", "graph")),
        P(("groups", "graph")),
        P(("groups", "graph")),
        P(("groups", "graph")),
        P(None, ("groups", "graph")),
        P(("groups", "graph")),
        P(),
        P(),
        P(),
        P(),
        P(),
        P(),
        P(),
    )
    return jax.shard_map(
        functools.partial(on_device, mesh.shape["graph"]),
        mesh=mesh,
        in_specs=placed,
        out_specs=(P(("groups", "graph"), None), P(("groups", "graph"), None)),
        check_vma=False,
    )
```

```python
import functools

import jax
import jax.numpy as jnp
from jax import lax
from jax.experimental import pallas as pl
from jax.experimental.pallas import tpu as pltpu
from jax.sharding import PartitionSpec as P

WIN = 512
HALVES = 2


inv_root = 0.7071067811865476


def matmul(left, right):
    return jnp.dot(left, right, preferred_element_type=jnp.float32)


def pick_rows(indices, table):
    chooser = (indices[:, None] == jnp.arange(table.shape[0], dtype=jnp.int32)[None, :]).astype(
        table.dtype
    )
    return matmul(chooser, table).astype(table.dtype)


def bilinear_terms(inputs_x, coeffs, keeps, w_bilinear):
    expanded = matmul(inputs_x, w_bilinear)
    expanded = expanded.reshape(inputs_x.shape[0], coeffs.shape[0], -1)
    mixed = jnp.einsum("tkd,kt->td", expanded, coeffs.astype(jnp.float32))
    return mixed * keeps.astype(jnp.float32)[:, None]


def tile_sums(slot_rows, local_in, local_out, keeps, coeffs, w_bilinear):
    trip_count = slot_rows.shape[0]
    block_size = WIN
    block_count = trip_count // block_size
    basis_rows = coeffs.shape[0]
    block_iota = jnp.arange(block_size, dtype=jnp.int32)

    def one_block(operands):
        rows_blk, in_blk, out_blk, keep_blk, coef_blk = operands
        in_hot = ((in_blk % block_size)[:, None] == block_iota[None, :]).astype(jnp.bfloat16)
        inputs_x = matmul(in_hot, rows_blk).astype(jnp.bfloat16)
        mixed = bilinear_terms(inputs_x, coef_blk, keep_blk, w_bilinear)
        out_hot = (block_iota[:, None] == (out_blk % block_size)[None, :]).astype(jnp.float32)
        return jnp.dot(
            out_hot, mixed, precision=lax.Precision.HIGHEST, preferred_element_type=jnp.float32
        )

    shaped_coeffs = jnp.transpose(coeffs.reshape(basis_rows, block_count, block_size), (1, 0, 2))
    summed = lax.map(
        one_block,
        (
            slot_rows.reshape(block_count, block_size, -1),
            local_in.reshape(block_count, block_size),
            local_out.reshape(block_count, block_size),
            keeps.reshape(block_count, block_size),
            shaped_coeffs,
        ),
    )
    return summed.reshape(trip_count, -1).astype(jnp.bfloat16)


def plain_on_device(
    edge_state,
    atom_state,
    atom_sends,
    edge_source,
    edge_target,
    send_edges,
    triplet_in,
    triplet_out,
    triplet_valid,
    triplet_basis,
    return_edges,
    w_edge,
    w_source,
    w_down,
    w_bilinear,
    w_up,
    w_residual,
    w_atom,
):
    edge_count = edge_state.shape[0]
    atom_count = atom_state.shape[0]
    arrived_atoms = lax.all_to_all(
        pick_rows(atom_sends, atom_state), "graph", split_axis=0, concat_axis=0, tiled=True
    )
    src_rows = pick_rows(edge_source, arrived_atoms)
    pre_act = matmul(edge_state, w_edge) + matmul(src_rows, w_source)
    activated = jax.nn.silu(pre_act).astype(jnp.bfloat16)
    projected = jax.nn.silu(matmul(activated, w_down)).astype(jnp.bfloat16)
    slot_rows = lax.all_to_all(
        pick_rows(send_edges, projected), "graph", split_axis=0, concat_axis=0, tiled=True
    )
    slot_sums = tile_sums(
        slot_rows, triplet_in, triplet_out, triplet_valid, triplet_basis, w_bilinear
    )
    returned = lax.all_to_all(slot_sums, "graph", split_axis=0, concat_axis=0, tiled=True)
    back_hot = (jnp.arange(edge_count, dtype=jnp.int32)[:, None] == return_edges[None, :]).astype(
        jnp.bfloat16
    )
    aggregate = matmul(back_hot, returned)
    update = jax.nn.silu(matmul(aggregate.astype(jnp.bfloat16), w_up))
    base = ((edge_state.astype(jnp.float32) + activated.astype(jnp.float32)) * inv_root).astype(
        jnp.bfloat16
    )
    inner_one = jax.nn.silu(matmul(base, w_residual[0])).astype(jnp.bfloat16)
    middle = (
        (base.astype(jnp.float32) + jax.nn.silu(matmul(inner_one, w_residual[1]))) * inv_root
    ).astype(jnp.bfloat16)
    inner_two = jax.nn.silu(matmul(middle, w_residual[2])).astype(jnp.bfloat16)
    chain = (middle.astype(jnp.float32) + jax.nn.silu(matmul(inner_two, w_residual[3]))) * inv_root
    edge_out = (chain + update).astype(jnp.bfloat16)
    contrib = matmul(edge_out, w_atom).astype(jnp.bfloat16)
    one_hot = (edge_target[None, :] == jnp.arange(atom_count, dtype=jnp.int32)[:, None]).astype(
        jnp.bfloat16
    )
    atom_sum = matmul(one_hot, contrib)
    atom_out = (atom_state.astype(jnp.float32) + jax.nn.silu(0.25 * atom_sum)).astype(jnp.bfloat16)
    return (edge_out, atom_out)


def silu(value):
    half = 0.5 * value
    return half + half * jnp.tanh(half)


def dot_at(left, right, left_dim, right_dim):
    return lax.dot_general(
        left, right, (((left_dim,), (right_dim,)), ((), ())), preferred_element_type=jnp.float32
    )


def hot_columns(row_count, indices):
    rows = lax.broadcasted_iota(jnp.int32, (row_count, indices.shape[1]), 0)
    return jnp.where(rows == indices, 1.0, 0.0).astype(jnp.bfloat16)


def partner(me, step, n):
    peer = me
    bit = 1
    while bit < n:
        mine = lax.rem(lax.div(me, bit), 2)
        flip = (step // bit) % 2 if isinstance(step, int) else lax.rem(lax.div(step, bit), 2)
        peer = peer + flip * (1 - 2 * mine) * bit
        bit *= 2
    return peer


def look_up(table, indices):
    lanes = indices.shape[1]
    found = []
    for row in range(indices.shape[0]):
        wanted = jnp.broadcast_to(indices[row : row + 1, :], (8, lanes))
        lane = wanted & (lanes - 1)
        value = jnp.zeros_like(wanted)
        for first in range(0, table.shape[1], lanes):
            part = jnp.take_along_axis(
                jnp.broadcast_to(table[:, first : first + lanes], (8, lanes)),
                lane,
                axis=1,
                mode="promise_in_bounds",
            )
            value = jnp.where(wanted - lane == first, part, value)
        found.append(value)
    return jnp.concatenate(found, axis=1)


def pick_columns(table, indices):
    lanes = 128
    found = []
    for start in range(0, indices.shape[1], lanes):
        wanted = indices[:, start : start + lanes]
        lane = wanted & (lanes - 1)
        blocks = []
        for row in range(0, table.shape[0], 8):
            value = None
            for first in range(0, table.shape[1], lanes):
                part = jnp.take_along_axis(
                    table[row : row + 8, first : first + lanes],
                    lane,
                    axis=1,
                    mode="promise_in_bounds",
                )
                value = part if value is None else jnp.where(wanted - lane == first, part, value)
            blocks.append(value)
        found.append(jnp.concatenate(blocks, axis=0))
    return jnp.concatenate(found, axis=1)


def hot_from(row_count, eight_rows):
    lanes = eight_rows.shape[1]
    sixteen = jnp.concatenate([eight_rows] * 2, axis=0).astype(jnp.int16)
    rows = lax.broadcasted_iota(jnp.int32, (row_count, 128), 0).astype(jnp.int16)
    spread = jnp.concatenate([sixteen] * (row_count // 16), axis=0)
    rows = jnp.concatenate([rows] * (lanes // 128), axis=1)
    return jnp.where(rows == spread, jnp.bfloat16(1.0), jnp.bfloat16(0.0))


def finish(total, chain, atom, target, w_up, w_atom):
    update = silu(dot_at(total.astype(jnp.bfloat16), w_up, 0, 0))
    edge_out = (chain + update).astype(jnp.bfloat16)
    contrib = matmul(edge_out, w_atom).astype(jnp.bfloat16)
    atom_sum = matmul(hot_columns(atom.shape[0], target), contrib)
    atom_out = (atom.astype(jnp.float32) + silu(0.25 * atom_sum)).astype(jnp.bfloat16)
    return edge_out, atom_out


def put_out(edge_v, atom_v, edge_out, atom_out, sem):
    puts = [
        pltpu.make_async_copy(edge_v, edge_out, sem.at[0]),
        pltpu.make_async_copy(atom_v, atom_out, sem.at[1]),
    ]
    for put in puts:
        put.start()
    for put in puts:
        put.wait()


def block_kernel(n, loaded, *refs):
    sources = refs[:loaded]
    in_hbm, out_hbm, valid_hbm, basis_hbm = refs[loaded : loaded + 4]
    edge_out_ref, atom_out_ref = refs[loaded + 4 : loaded + 6]
    held = refs[loaded + 6 : 2 * loaded + 6]
    (
        stage_v,
        valid_v,
        stage_basis_v,
        ends_out,
        ends_v,
        basis_out,
        basis_v,
        atoms_out,
        atoms_in,
        weight_v,
        rows_even,
        rows_odd,
        hots_even,
        hots_odd,
        chain_v,
        sum_v,
        load_sem,
        stage_sem,
        send_sem,
        recv_sem,
        ready,
    ) = refs[2 * loaded + 6 :]
    (
        atom_v,
        asend_v,
        edge_v,
        w_edge_v,
        source_v,
        w_source_v,
        w_down_v,
        w_bilinear_v,
        w_res_v,
        send_v,
        return_v,
        target_v,
        w_up_v,
        w_atom_v,
    ) = held
    me = lax.axis_index("graph")
    cap = basis_v.shape[2]
    rows = ends_v.shape[1] // 2
    edge_count = edge_v.shape[0]
    width = w_down_v.shape[0]
    basis_count = basis_v.shape[1]
    bf16 = jnp.bfloat16
    layers = ready.shape[0]
    span = n // layers
    layer = lax.div(me, span)
    rows_v = (rows_even, rows_odd)
    hots_v = (hots_even, hots_odd)
    arrays = (ends_v, basis_v, atoms_in)
    sources_of = (ends_out, basis_out, atoms_out)

    def signal(semaphore, peer):
        pl.semaphore_signal(
            semaphore, inc=1, device_id={"graph": peer}, device_id_type=pl.DeviceIdType.MESH
        )

    barrier = pltpu.get_barrier_semaphore()
    loads = [
        pltpu.make_async_copy(src, dst, load_sem.at[i])
        for i, (src, dst) in enumerate(zip(sources, held))
    ]
    stages = [
        pltpu.make_async_copy(src, dst, stage_sem.at[i])
        for i, (src, dst) in enumerate(
            (
                (in_hbm, stage_v.at[:, pl.ds(0, rows)]),
                (out_hbm, stage_v.at[:, pl.ds(rows, rows)]),
                (valid_hbm, valid_v),
                (basis_hbm, stage_basis_v),
            )
        )
    ]
    for load in loads[:2]:
        load.start()
    for stage in stages:
        stage.start()
    for peer in range(n):
        pl.when((layer <= peer // span) & (me != peer))(functools.partial(signal, barrier, peer))
    for load in loads[2:]:
        load.start()
    pl.semaphore_wait(barrier, span * (layer + 1) - 1)
    for peer in range(n):
        pl.when(layer > peer // span)(functools.partial(signal, ready.at[layer], peer))
    loads[0].wait()
    loads[1].wait()
    picked = dot_at(hot_columns(atom_v.shape[0], asend_v[...]), atom_v[...], 0, 0)
    atoms_out[...] = picked.reshape(atoms_out.shape).astype(bf16)
    def own(kind):
        pltpu.make_async_copy(
            sources_of[kind].at[me], arrays[kind].at[me], recv_sem.at[kind, 0]
        ).start()

    inner = lax.rem(me, span)

    def send(kinds, other):
        apart = partner(layer, other, layers)
        for step in range(span):
            peer = other * span + partner(inner, step, span)

            def start():
                for kind in kinds:
                    pltpu.make_async_remote_copy(
                        src_ref=sources_of[kind].at[peer],
                        dst_ref=arrays[kind].at[me],
                        send_sem=send_sem.at[kind],
                        recv_sem=recv_sem.at[kind, 0 if kind == 2 else apart],
                        device_id={"graph": peer},
                        device_id_type=pl.DeviceIdType.MESH,
                    ).start()

            if step:
                start()
            else:
                pl.when(layer != other)(start)

    def arrive(buffer, sem):
        pltpu.make_async_copy(buffer, buffer, sem).wait()

    own(2)
    for other in range(layers):

        @pl.when(layer >= other)
        def _():
            send((2,), other)

    for stage in stages:
        stage.wait()
    ends_out[...] = stage_v[...].astype(jnp.int16)
    for tile in range(n):
        basis_out[tile] = stage_basis_v[:, tile * cap : (tile + 1) * cap] * valid_v[tile].astype(
            jnp.float32
        ).astype(bf16)
    own(0)
    own(1)
    for other in range(layers):

        @pl.when(layer == other)
        def _():
            send((0, 1), other)

    for other in range(layers):

        @pl.when(layer > other)
        def _():
            send((0, 1), other)

    for load in loads[2:8]:
        load.wait()
    weight_v[...] = jnp.concatenate(
        [w_bilinear_v[:, k * width : (k + 1) * width] for k in range(basis_count)], axis=0
    ).T
    edge = edge_v[...]
    pre_act = matmul(edge, w_edge_v[...])
    pick = hot_columns(atoms_in.shape[0] * atoms_in.shape[1], source_v[...])
    for load in loads[8:]:
        load.wait()
    for other in range(1, layers):

        @pl.when(layer < other)
        def _():
            pl.semaphore_wait(ready.at[other], span)
            send((2,), other)

    for other in (layers - 1, *range(1, layers - 1)):

        @pl.when(layer < other)
        def _():
            send((0, 1), other)

    arrive(atoms_in, recv_sem.at[2, 0])
    for kind, buffer in enumerate(arrays[:2]):
        arrive(buffer.at[pl.ds(layer * span, span)], recv_sem.at[kind, 0])
    arrived = atoms_in[...].astype(jnp.float32).reshape(pick.shape[0], -1).astype(bf16)
    src_rows = dot_at(pick, arrived, 0, 0).astype(bf16)
    activated = silu(pre_act + matmul(src_rows, w_source_v[...])).astype(bf16)
    projected = silu(dot_at(w_down_v[...], activated, 1, 1)).astype(bf16)
    base = ((edge.astype(jnp.float32) + activated.astype(jnp.float32)) * inv_root).astype(bf16)
    inner_one = silu(matmul(base, w_res_v[0])).astype(bf16)
    middle = ((base.astype(jnp.float32) + silu(matmul(inner_one, w_res_v[1]))) * inv_root).astype(bf16)
    inner_two = silu(matmul(middle, w_res_v[2])).astype(bf16)
    chain_v[...] = (middle.astype(jnp.float32) + silu(matmul(inner_two, w_res_v[3]))) * inv_root

    def first_of(apart):
        return partner(layer, apart, layers) * span

    def prepare(apart):
        for i in range(span):
            tile = first_of(apart) + i
            ends = ends_v[tile].astype(jnp.int32) & (cap - 1)
            edges = look_up(send_v[tile], ends[:rows])
            rows_v[apart % 2][i] = pick_columns(projected.astype(jnp.float32), edges).astype(bf16)
            targets = look_up(return_v[tile], ends[rows:])
            hots_v[apart % 2][i] = hot_from(edge_count, targets)

    def add_terms(apart):
        share = basis_count // HALVES
        hots = jnp.concatenate([hots_v[apart % 2][i] for i in range(span)], axis=1)
        for half in range(HALVES):
            all_terms = []
            for i in range(span):
                gathered = rows_v[apart % 2][i]
                coeffs = basis_v[first_of(apart) + i].astype(jnp.float32)
                terms = []
                for k in range(half * share, (half + 1) * share):
                    spread = jnp.broadcast_to(coeffs[k : k + 1, :], (16, cap)).astype(bf16)
                    terms.append(jnp.concatenate([spread] * (width // 16), axis=0) * gathered)
                all_terms.append(jnp.concatenate(terms, axis=0))
            part = dot_at(jnp.concatenate(all_terms, axis=1), hots, 1, 1)
            slots = pl.ds(half * share * width, share * width)
            if apart:
                sum_v[slots, :] += part
            else:
                sum_v[slots, :] = part

    def arrived_from(apart):
        for kind, buffer in enumerate(arrays[:2]):
            arrive(buffer.at[pl.ds(first_of(apart), span)], recv_sem.at[kind, apart])

    prepare(0)
    for apart in range(layers):
        add_terms(apart)
        if apart + 1 < layers:
            arrived_from(apart + 1)
            prepare(apart + 1)
    total = matmul(weight_v[...], sum_v[...].astype(bf16))
    edge_out, atom_out = finish(
        total, chain_v[...], atom_v[...], target_v[...], w_up_v[...], w_atom_v[...]
    )
    edge_out_ref[...] = edge_out
    atom_out_ref[...] = atom_out
    for kind, buffer in enumerate(arrays):
        arrive(buffer.at[pl.ds(0, n - 1)], send_sem.at[kind])


def on_device(
    n,
    edge_state,
    atom_state,
    atom_sends,
    edge_source,
    edge_target,
    send_edges,
    triplet_in,
    triplet_out,
    triplet_valid,
    triplet_basis,
    return_edges,
    w_edge,
    w_source,
    w_down,
    w_bilinear,
    w_up,
    w_residual,
    w_atom,
):
    cap = triplet_in.shape[0] // n
    layers = 4
    if cap % WIN or cap & (cap - 1) or n & (n - 1) or n < layers:
        return plain_on_device(
            edge_state,
            atom_state,
            atom_sends,
            edge_source,
            edge_target,
            send_edges,
            triplet_in,
            triplet_out,
            triplet_valid,
            triplet_basis,
            return_edges,
            w_edge,
            w_source,
            w_down,
            w_bilinear,
            w_up,
            w_residual,
            w_atom,
        )
    edge_count, edge_width = edge_state.shape
    atom_count, atom_width = atom_state.shape
    basis_count = triplet_basis.shape[0]
    width = w_down.shape[1]
    slots = atom_sends.shape[0] // n
    bf16 = jnp.bfloat16
    loaded = (
        atom_state,
        atom_sends.reshape(1, -1),
        edge_state,
        w_edge,
        edge_source.reshape(1, -1),
        w_source,
        w_down.T,
        w_bilinear,
        w_residual,
        send_edges.reshape(n, 1, cap),
        return_edges.reshape(n, 1, cap),
        edge_target.reshape(1, -1),
        w_up,
        w_atom,
    )
    whole = pl.BlockSpec(memory_space=pltpu.VMEM)
    edge_out, atom_out = pl.pallas_call(
        functools.partial(block_kernel, n, len(loaded)),
        out_shape=(
            pltpu.VMEM((edge_count, edge_width), bf16),
            pltpu.VMEM((atom_count, atom_width), bf16),
        ),
        in_specs=[pl.BlockSpec(memory_space=pl.ANY)] * (len(loaded) + 4),
        out_specs=(whole, whole),
        scratch_shapes=[pltpu.VMEM(each.shape, each.dtype) for each in loaded]
        + [
            pltpu.VMEM((n, 2 * (cap // 128), 128), jnp.int32),
            pltpu.VMEM((n, 1, cap), jnp.int32),
            pltpu.VMEM(triplet_basis.shape, bf16),
            pltpu.VMEM((n, 2 * (cap // 128), 128), jnp.int16),
            pltpu.VMEM((n, 2 * (cap // 128), 128), jnp.int16),
            pltpu.VMEM((n, basis_count, cap), bf16),
            pltpu.VMEM((n, basis_count, cap), bf16),
            pltpu.VMEM((n, slots, atom_width), bf16),
            pltpu.VMEM((n, slots, atom_width), bf16),
            pltpu.VMEM((width, basis_count * width), bf16),
            pltpu.VMEM((n // layers, width, cap), bf16),
            pltpu.VMEM((n // layers, width, cap), bf16),
            pltpu.VMEM((n // layers, edge_count, cap), bf16),
            pltpu.VMEM((n // layers, edge_count, cap), bf16),
            pltpu.VMEM((edge_count, edge_width), jnp.float32),
            pltpu.VMEM((basis_count * width, edge_count), jnp.float32),
            pltpu.SemaphoreType.DMA((len(loaded),)),
            pltpu.SemaphoreType.DMA((4,)),
            pltpu.SemaphoreType.DMA((3,)),
            pltpu.SemaphoreType.DMA((3, layers)),
            pltpu.SemaphoreType.REGULAR((layers,)),
        ],
        compiler_params=pltpu.CompilerParams(collective_id=0, has_side_effects=True),
        name="block",
    )(
        *loaded,
        triplet_in.reshape(n, cap // 128, 128),
        triplet_out.reshape(n, cap // 128, 128),
        triplet_valid.reshape(n, 1, cap),
        triplet_basis,
    )
    return pl.pallas_call(
        put_out,
        out_shape=(
            jax.ShapeDtypeStruct(edge_out.shape, bf16),
            jax.ShapeDtypeStruct(atom_out.shape, bf16),
        ),
        in_specs=[whole, whole],
        out_specs=(pl.BlockSpec(memory_space=pl.ANY),) * 2,
        scratch_shapes=[pltpu.SemaphoreType.DMA((2,))],
        name="tail",
    )(
        pltpu.with_memory_space_constraint(edge_out, pltpu.VMEM),
        pltpu.with_memory_space_constraint(atom_out, pltpu.VMEM),
    )


def solution(mesh):
    placed = (
        P(("groups", "graph"), None),
        P(("groups", "graph"), None),
        P(("groups", "graph")),
        P(("groups", "graph")),
        P(("groups", "graph")),
        P(("groups", "graph")),
        P(("groups", "graph")),
        P(("groups", "graph")),
        P(("groups", "graph")),
        P(None, ("groups", "graph")),
        P(("groups", "graph")),
        P(),
        P(),
        P(),
        P(),
        P(),
        P(),
        P(),
    )
    return jax.shard_map(
        functools.partial(on_device, mesh.shape["graph"]),
        mesh=mesh,
        in_specs=placed,
        out_specs=(P(("groups", "graph"), None), P(("groups", "graph"), None)),
        check_vma=False,
    )
```

```python
import functools

import jax
import jax.numpy as jnp
from jax import lax
from jax.experimental import pallas as pl
from jax.experimental.pallas import tpu as pltpu
from jax.sharding import PartitionSpec as P

WIN = 512
HALVES = 2


inv_root = 0.7071067811865476


def matmul(left, right):
    return jnp.dot(left, right, preferred_element_type=jnp.float32)


def pick_rows(indices, table):
    chooser = (indices[:, None] == jnp.arange(table.shape[0], dtype=jnp.int32)[None, :]).astype(
        table.dtype
    )
    return matmul(chooser, table).astype(table.dtype)


def bilinear_terms(inputs_x, coeffs, keeps, w_bilinear):
    expanded = matmul(inputs_x, w_bilinear)
    expanded = expanded.reshape(inputs_x.shape[0], coeffs.shape[0], -1)
    mixed = jnp.einsum("tkd,kt->td", expanded, coeffs.astype(jnp.float32))
    return mixed * keeps.astype(jnp.float32)[:, None]


def tile_sums(slot_rows, local_in, local_out, keeps, coeffs, w_bilinear):
    trip_count = slot_rows.shape[0]
    block_size = WIN
    block_count = trip_count // block_size
    basis_rows = coeffs.shape[0]
    block_iota = jnp.arange(block_size, dtype=jnp.int32)

    def one_block(operands):
        rows_blk, in_blk, out_blk, keep_blk, coef_blk = operands
        in_hot = ((in_blk % block_size)[:, None] == block_iota[None, :]).astype(jnp.bfloat16)
        inputs_x = matmul(in_hot, rows_blk).astype(jnp.bfloat16)
        mixed = bilinear_terms(inputs_x, coef_blk, keep_blk, w_bilinear)
        out_hot = (block_iota[:, None] == (out_blk % block_size)[None, :]).astype(jnp.float32)
        return jnp.dot(
            out_hot, mixed, precision=lax.Precision.HIGHEST, preferred_element_type=jnp.float32
        )

    shaped_coeffs = jnp.transpose(coeffs.reshape(basis_rows, block_count, block_size), (1, 0, 2))
    summed = lax.map(
        one_block,
        (
            slot_rows.reshape(block_count, block_size, -1),
            local_in.reshape(block_count, block_size),
            local_out.reshape(block_count, block_size),
            keeps.reshape(block_count, block_size),
            shaped_coeffs,
        ),
    )
    return summed.reshape(trip_count, -1).astype(jnp.bfloat16)


def plain_on_device(
    edge_state,
    atom_state,
    atom_sends,
    edge_source,
    edge_target,
    send_edges,
    triplet_in,
    triplet_out,
    triplet_valid,
    triplet_basis,
    return_edges,
    w_edge,
    w_source,
    w_down,
    w_bilinear,
    w_up,
    w_residual,
    w_atom,
):
    edge_count = edge_state.shape[0]
    atom_count = atom_state.shape[0]
    arrived_atoms = lax.all_to_all(
        pick_rows(atom_sends, atom_state), "graph", split_axis=0, concat_axis=0, tiled=True
    )
    src_rows = pick_rows(edge_source, arrived_atoms)
    pre_act = matmul(edge_state, w_edge) + matmul(src_rows, w_source)
    activated = jax.nn.silu(pre_act).astype(jnp.bfloat16)
    projected = jax.nn.silu(matmul(activated, w_down)).astype(jnp.bfloat16)
    slot_rows = lax.all_to_all(
        pick_rows(send_edges, projected), "graph", split_axis=0, concat_axis=0, tiled=True
    )
    slot_sums = tile_sums(
        slot_rows, triplet_in, triplet_out, triplet_valid, triplet_basis, w_bilinear
    )
    returned = lax.all_to_all(slot_sums, "graph", split_axis=0, concat_axis=0, tiled=True)
    back_hot = (jnp.arange(edge_count, dtype=jnp.int32)[:, None] == return_edges[None, :]).astype(
        jnp.bfloat16
    )
    aggregate = matmul(back_hot, returned)
    update = jax.nn.silu(matmul(aggregate.astype(jnp.bfloat16), w_up))
    base = ((edge_state.astype(jnp.float32) + activated.astype(jnp.float32)) * inv_root).astype(
        jnp.bfloat16
    )
    inner_one = jax.nn.silu(matmul(base, w_residual[0])).astype(jnp.bfloat16)
    middle = (
        (base.astype(jnp.float32) + jax.nn.silu(matmul(inner_one, w_residual[1]))) * inv_root
    ).astype(jnp.bfloat16)
    inner_two = jax.nn.silu(matmul(middle, w_residual[2])).astype(jnp.bfloat16)
    chain = (middle.astype(jnp.float32) + jax.nn.silu(matmul(inner_two, w_residual[3]))) * inv_root
    edge_out = (chain + update).astype(jnp.bfloat16)
    contrib = matmul(edge_out, w_atom).astype(jnp.bfloat16)
    one_hot = (edge_target[None, :] == jnp.arange(atom_count, dtype=jnp.int32)[:, None]).astype(
        jnp.bfloat16
    )
    atom_sum = matmul(one_hot, contrib)
    atom_out = (atom_state.astype(jnp.float32) + jax.nn.silu(0.25 * atom_sum)).astype(jnp.bfloat16)
    return (edge_out, atom_out)


def silu(value):
    half = 0.5 * value
    return half + half * jnp.tanh(half)


def dot_at(left, right, left_dim, right_dim):
    return lax.dot_general(
        left, right, (((left_dim,), (right_dim,)), ((), ())), preferred_element_type=jnp.float32
    )


def hot_columns(row_count, indices):
    rows = lax.broadcasted_iota(jnp.int32, (row_count, indices.shape[1]), 0)
    return jnp.where(rows == indices, 1.0, 0.0).astype(jnp.bfloat16)


def partner(me, step, n):
    peer = me
    bit = 1
    while bit < n:
        mine = lax.rem(lax.div(me, bit), 2)
        flip = (step // bit) % 2 if isinstance(step, int) else lax.rem(lax.div(step, bit), 2)
        peer = peer + flip * (1 - 2 * mine) * bit
        bit *= 2
    return peer


def look_up(table, indices):
    lanes = indices.shape[1]
    found = []
    for row in range(indices.shape[0]):
        wanted = jnp.broadcast_to(indices[row : row + 1, :], (8, lanes))
        lane = wanted & (lanes - 1)
        value = jnp.zeros_like(wanted)
        for first in range(0, table.shape[1], lanes):
            part = jnp.take_along_axis(
                jnp.broadcast_to(table[:, first : first + lanes], (8, lanes)),
                lane,
                axis=1,
                mode="promise_in_bounds",
            )
            value = jnp.where(wanted - lane == first, part, value)
        found.append(value)
    return jnp.concatenate(found, axis=1)


def pick_columns(table, indices):
    lanes = 128
    found = []
    for start in range(0, indices.shape[1], lanes):
        wanted = indices[:, start : start + lanes]
        lane = wanted & (lanes - 1)
        blocks = []
        for row in range(0, table.shape[0], 8):
            value = None
            for first in range(0, table.shape[1], lanes):
                part = jnp.take_along_axis(
                    table[row : row + 8, first : first + lanes],
                    lane,
                    axis=1,
                    mode="promise_in_bounds",
                )
                value = part if value is None else jnp.where(wanted - lane == first, part, value)
            blocks.append(value)
        found.append(jnp.concatenate(blocks, axis=0))
    return jnp.concatenate(found, axis=1)


def hot_from(row_count, eight_rows):
    lanes = eight_rows.shape[1]
    sixteen = jnp.concatenate([eight_rows] * 2, axis=0).astype(jnp.int16)
    rows = lax.broadcasted_iota(jnp.int32, (row_count, 128), 0).astype(jnp.int16)
    spread = jnp.concatenate([sixteen] * (row_count // 16), axis=0)
    rows = jnp.concatenate([rows] * (lanes // 128), axis=1)
    return jnp.where(rows == spread, jnp.bfloat16(1.0), jnp.bfloat16(0.0))


def finish(total, chain, atom, target, w_up, w_atom):
    update = silu(dot_at(total.astype(jnp.bfloat16), w_up, 0, 0))
    edge_out = (chain + update).astype(jnp.bfloat16)
    contrib = matmul(edge_out, w_atom).astype(jnp.bfloat16)
    atom_sum = matmul(hot_columns(atom.shape[0], target), contrib)
    atom_out = (atom.astype(jnp.float32) + silu(0.25 * atom_sum)).astype(jnp.bfloat16)
    return edge_out, atom_out


def put_out(edge_v, atom_v, edge_out, atom_out, sem):
    puts = [
        pltpu.make_async_copy(edge_v, edge_out, sem.at[0]),
        pltpu.make_async_copy(atom_v, atom_out, sem.at[1]),
    ]
    for put in puts:
        put.start()
    for put in puts:
        put.wait()


def block_kernel(n, loaded, *refs):
    sources = refs[:loaded]
    in_hbm, out_hbm, valid_hbm, basis_hbm = refs[loaded : loaded + 4]
    edge_out_ref, atom_out_ref = refs[loaded + 4 : loaded + 6]
    held = refs[loaded + 6 : 2 * loaded + 6]
    (
        stage_v,
        valid_v,
        stage_basis_v,
        ends_out,
        ends_v,
        basis_out,
        basis_v,
        atoms_out,
        atoms_in,
        weight_v,
        rows_even,
        rows_odd,
        hots_even,
        hots_odd,
        edges_v,
        chain_v,
        sum_v,
        load_sem,
        stage_sem,
        send_sem,
        recv_sem,
        ready,
    ) = refs[2 * loaded + 6 :]
    (
        atom_v,
        asend_v,
        edge_v,
        w_edge_v,
        source_v,
        w_source_v,
        w_down_v,
        w_bilinear_v,
        w_res_v,
        send_v,
        return_v,
        target_v,
        w_up_v,
        w_atom_v,
    ) = held
    me = lax.axis_index("graph")
    cap = basis_v.shape[2]
    rows = ends_v.shape[1] // 2
    edge_count = edge_v.shape[0]
    width = w_down_v.shape[0]
    basis_count = basis_v.shape[1]
    bf16 = jnp.bfloat16
    layers = ready.shape[0]
    span = n // layers
    layer = lax.div(me, span)
    rows_v = (rows_even, rows_odd)
    hots_v = (hots_even, hots_odd)
    arrays = (ends_v, basis_v, atoms_in)
    sources_of = (ends_out, basis_out, atoms_out)

    def signal(semaphore, peer):
        pl.semaphore_signal(
            semaphore, inc=1, device_id={"graph": peer}, device_id_type=pl.DeviceIdType.MESH
        )

    barrier = pltpu.get_barrier_semaphore()
    loads = [
        pltpu.make_async_copy(src, dst, load_sem.at[i])
        for i, (src, dst) in enumerate(zip(sources, held))
    ]
    stages = [
        pltpu.make_async_copy(src, dst, stage_sem.at[i])
        for i, (src, dst) in enumerate(
            (
                (in_hbm, stage_v.at[:, pl.ds(0, rows)]),
                (out_hbm, stage_v.at[:, pl.ds(rows, rows)]),
                (valid_hbm, valid_v),
                (basis_hbm, stage_basis_v),
            )
        )
    ]
    for load in loads[:2]:
        load.start()
    for stage in stages:
        stage.start()
    for peer in range(n):
        pl.when((layer <= peer // span) & (me != peer))(functools.partial(signal, barrier, peer))
    for load in loads[2:]:
        load.start()
    pl.semaphore_wait(barrier, span * (layer + 1) - 1)
    for peer in range(n):
        pl.when(layer > peer // span)(functools.partial(signal, ready.at[layer], peer))
    loads[0].wait()
    loads[1].wait()
    picked = dot_at(hot_columns(atom_v.shape[0], asend_v[...]), atom_v[...], 0, 0)
    atoms_out[...] = picked.reshape(atoms_out.shape).astype(bf16)
    def own(kind):
        pltpu.make_async_copy(
            sources_of[kind].at[me], arrays[kind].at[me], recv_sem.at[kind, 0]
        ).start()

    inner = lax.rem(me, span)

    def send(kinds, other):
        apart = partner(layer, other, layers)
        for step in range(span):
            peer = other * span + partner(inner, step, span)

            def start():
                for kind in kinds:
                    pltpu.make_async_remote_copy(
                        src_ref=sources_of[kind].at[peer],
                        dst_ref=arrays[kind].at[me],
                        send_sem=send_sem.at[kind],
                        recv_sem=recv_sem.at[kind, 0 if kind == 2 else apart],
                        device_id={"graph": peer},
                        device_id_type=pl.DeviceIdType.MESH,
                    ).start()

            if step:
                start()
            else:
                pl.when(layer != other)(start)

    def arrive(buffer, sem):
        pltpu.make_async_copy(buffer, buffer, sem).wait()

    own(2)
    for other in range(layers):

        @pl.when(layer >= other)
        def _():
            send((2,), other)

    for stage in stages:
        stage.wait()
    ends_out[...] = stage_v[...].astype(jnp.int16)
    for other in range(layers):
        for tile in range(other * span, (other + 1) * span):
            basis_out[tile] = stage_basis_v[:, tile * cap : (tile + 1) * cap] * valid_v[
                tile
            ].astype(jnp.float32).astype(bf16)

        @pl.when(layer == other)
        def _():
            own(0)
            own(1)

        @pl.when(layer >= other)
        def _():
            send((0, 1), other)

    for load in loads[2:8]:
        load.wait()
    weight_v[...] = jnp.concatenate(
        [w_bilinear_v[:, k * width : (k + 1) * width] for k in range(basis_count)], axis=0
    ).T
    edge = edge_v[...]
    pre_act = matmul(edge, w_edge_v[...])
    pick = hot_columns(atoms_in.shape[0] * atoms_in.shape[1], source_v[...])
    for load in loads[8:]:
        load.wait()
    def first_of(apart):
        return partner(layer, apart, layers) * span

    def find(apart):
        for i in range(span):
            tile = first_of(apart) + i
            ends = ends_v[tile].astype(jnp.int32) & (cap - 1)
            edges_v[apart % 2, i] = look_up(send_v[tile], ends[:rows])
            targets = look_up(return_v[tile], ends[rows:])
            hots_v[apart % 2][i] = hot_from(edge_count, targets)

    for other in range(1, layers):

        @pl.when(layer < other)
        def _():
            pl.semaphore_wait(ready.at[other], span)
            send((2,), other)

    for other in (layers - 1, *range(1, layers - 1)):

        @pl.when(layer < other)
        def _():
            send((0, 1), other)

    for kind, buffer in enumerate(arrays[:2]):
        arrive(buffer.at[pl.ds(layer * span, span)], recv_sem.at[kind, 0])
    find(0)
    arrive(atoms_in, recv_sem.at[2, 0])
    arrived = atoms_in[...].astype(jnp.float32).reshape(pick.shape[0], -1).astype(bf16)
    src_rows = dot_at(pick, arrived, 0, 0).astype(bf16)
    activated = silu(pre_act + matmul(src_rows, w_source_v[...])).astype(bf16)
    projected = silu(dot_at(w_down_v[...], activated, 1, 1)).astype(bf16)
    base = ((edge.astype(jnp.float32) + activated.astype(jnp.float32)) * inv_root).astype(bf16)
    inner_one = silu(matmul(base, w_res_v[0])).astype(bf16)
    middle = ((base.astype(jnp.float32) + silu(matmul(inner_one, w_res_v[1]))) * inv_root).astype(bf16)
    inner_two = silu(matmul(middle, w_res_v[2])).astype(bf16)
    chain_v[...] = (middle.astype(jnp.float32) + silu(matmul(inner_two, w_res_v[3]))) * inv_root

    def prepare(apart):
        if apart:
            find(apart)
        for i in range(span):
            rows_v[apart % 2][i] = pick_columns(
                projected.astype(jnp.float32), edges_v[apart % 2, i]
            ).astype(bf16)

    def add_terms(apart):
        share = basis_count // HALVES
        hots = jnp.concatenate([hots_v[apart % 2][i] for i in range(span)], axis=1)
        for half in range(HALVES):
            all_terms = []
            for i in range(span):
                gathered = rows_v[apart % 2][i]
                coeffs = basis_v[first_of(apart) + i].astype(jnp.float32)
                terms = []
                for k in range(half * share, (half + 1) * share):
                    spread = jnp.broadcast_to(coeffs[k : k + 1, :], (16, cap)).astype(bf16)
                    terms.append(jnp.concatenate([spread] * (width // 16), axis=0) * gathered)
                all_terms.append(jnp.concatenate(terms, axis=0))
            part = dot_at(jnp.concatenate(all_terms, axis=1), hots, 1, 1)
            slots = pl.ds(half * share * width, share * width)
            if apart:
                sum_v[slots, :] += part
            else:
                sum_v[slots, :] = part

    def arrived_from(apart):
        for kind, buffer in enumerate(arrays[:2]):
            arrive(buffer.at[pl.ds(first_of(apart), span)], recv_sem.at[kind, apart])

    prepare(0)
    for apart in range(layers):
        add_terms(apart)
        if apart + 1 < layers:
            arrived_from(apart + 1)
            prepare(apart + 1)
    total = matmul(weight_v[...], sum_v[...].astype(bf16))
    edge_out, atom_out = finish(
        total, chain_v[...], atom_v[...], target_v[...], w_up_v[...], w_atom_v[...]
    )
    edge_out_ref[...] = edge_out
    atom_out_ref[...] = atom_out
    for kind, buffer in enumerate(arrays):
        arrive(buffer.at[pl.ds(0, n - 1)], send_sem.at[kind])


def on_device(
    n,
    edge_state,
    atom_state,
    atom_sends,
    edge_source,
    edge_target,
    send_edges,
    triplet_in,
    triplet_out,
    triplet_valid,
    triplet_basis,
    return_edges,
    w_edge,
    w_source,
    w_down,
    w_bilinear,
    w_up,
    w_residual,
    w_atom,
):
    cap = triplet_in.shape[0] // n
    layers = 4
    if cap % WIN or cap & (cap - 1) or n & (n - 1) or n < layers:
        return plain_on_device(
            edge_state,
            atom_state,
            atom_sends,
            edge_source,
            edge_target,
            send_edges,
            triplet_in,
            triplet_out,
            triplet_valid,
            triplet_basis,
            return_edges,
            w_edge,
            w_source,
            w_down,
            w_bilinear,
            w_up,
            w_residual,
            w_atom,
        )
    edge_count, edge_width = edge_state.shape
    atom_count, atom_width = atom_state.shape
    basis_count = triplet_basis.shape[0]
    width = w_down.shape[1]
    slots = atom_sends.shape[0] // n
    bf16 = jnp.bfloat16
    loaded = (
        atom_state,
        atom_sends.reshape(1, -1),
        edge_state,
        w_edge,
        edge_source.reshape(1, -1),
        w_source,
        w_down.T,
        w_bilinear,
        w_residual,
        send_edges.reshape(n, 1, cap),
        return_edges.reshape(n, 1, cap),
        edge_target.reshape(1, -1),
        w_up,
        w_atom,
    )
    whole = pl.BlockSpec(memory_space=pltpu.VMEM)
    edge_out, atom_out = pl.pallas_call(
        functools.partial(block_kernel, n, len(loaded)),
        out_shape=(
            pltpu.VMEM((edge_count, edge_width), bf16),
            pltpu.VMEM((atom_count, atom_width), bf16),
        ),
        in_specs=[pl.BlockSpec(memory_space=pl.ANY)] * (len(loaded) + 4),
        out_specs=(whole, whole),
        scratch_shapes=[pltpu.VMEM(each.shape, each.dtype) for each in loaded]
        + [
            pltpu.VMEM((n, 2 * (cap // 128), 128), jnp.int32),
            pltpu.VMEM((n, 1, cap), jnp.int32),
            pltpu.VMEM(triplet_basis.shape, bf16),
            pltpu.VMEM((n, 2 * (cap // 128), 128), jnp.int16),
            pltpu.VMEM((n, 2 * (cap // 128), 128), jnp.int16),
            pltpu.VMEM((n, basis_count, cap), bf16),
            pltpu.VMEM((n, basis_count, cap), bf16),
            pltpu.VMEM((n, slots, atom_width), bf16),
            pltpu.VMEM((n, slots, atom_width), bf16),
            pltpu.VMEM((width, basis_count * width), bf16),
            pltpu.VMEM((n // layers, width, cap), bf16),
            pltpu.VMEM((n // layers, width, cap), bf16),
            pltpu.VMEM((n // layers, edge_count, cap), bf16),
            pltpu.VMEM((n // layers, edge_count, cap), bf16),
            pltpu.VMEM((2, n // layers, 8, cap), jnp.int32),
            pltpu.VMEM((edge_count, edge_width), jnp.float32),
            pltpu.VMEM((basis_count * width, edge_count), jnp.float32),
            pltpu.SemaphoreType.DMA((len(loaded),)),
            pltpu.SemaphoreType.DMA((4,)),
            pltpu.SemaphoreType.DMA((3,)),
            pltpu.SemaphoreType.DMA((3, layers)),
            pltpu.SemaphoreType.REGULAR((layers,)),
        ],
        compiler_params=pltpu.CompilerParams(collective_id=0, has_side_effects=True),
        name="block",
    )(
        *loaded,
        triplet_in.reshape(n, cap // 128, 128),
        triplet_out.reshape(n, cap // 128, 128),
        triplet_valid.reshape(n, 1, cap),
        triplet_basis,
    )
    return pl.pallas_call(
        put_out,
        out_shape=(
            jax.ShapeDtypeStruct(edge_out.shape, bf16),
            jax.ShapeDtypeStruct(atom_out.shape, bf16),
        ),
        in_specs=[whole, whole],
        out_specs=(pl.BlockSpec(memory_space=pl.ANY),) * 2,
        scratch_shapes=[pltpu.SemaphoreType.DMA((2,))],
        name="tail",
    )(
        pltpu.with_memory_space_constraint(edge_out, pltpu.VMEM),
        pltpu.with_memory_space_constraint(atom_out, pltpu.VMEM),
    )


def solution(mesh):
    placed = (
        P(("groups", "graph"), None),
        P(("groups", "graph"), None),
        P(("groups", "graph")),
        P(("groups", "graph")),
        P(("groups", "graph")),
        P(("groups", "graph")),
        P(("groups", "graph")),
        P(("groups", "graph")),
        P(("groups", "graph")),
        P(None, ("groups", "graph")),
        P(("groups", "graph")),
        P(),
        P(),
        P(),
        P(),
        P(),
        P(),
        P(),
    )
    return jax.shard_map(
        functools.partial(on_device, mesh.shape["graph"]),
        mesh=mesh,
        in_specs=placed,
        out_specs=(P(("groups", "graph"), None), P(("groups", "graph"), None)),
        check_vma=False,
    )
```
